16 devices in a mesh: rep: 1, dp: 16 (over x, y, z, core).
Axes of the slice: x: 2, y: 2, z: 2, core: 2. Of those that a mesh axis runs over, the one named last changes fastest.
Arguments:
- x: bfloat16 [16, 2048, 1024], P(('rep', 'dp'))
- dy: bfloat16 [16, 2048, 1024], P(('rep', 'dp'))
- w_gate: bfloat16 [2, 1024, 2560], P(None, 'dp')
- w_up: bfloat16 [2, 1024, 2560], P(None, 'dp')
- w_down: bfloat16 [2, 2560, 1024], P(None, 'dp')
Outputs:
- output 1: bfloat16 [16, 2048, 1024], P(('rep', 'dp'))
- output 2: bfloat16 [2, 1024, 2560], P('rep', 'dp')
- output 3: bfloat16 [2, 1024, 2560], P('rep', 'dp')
- output 4: bfloat16 [2, 2560, 1024], P('rep', 'dp')
All inputs are finite; a program needn't handle non-finite values.
Results may differ from the reference program's by a relative error of at most 0.018.
Values are sent between devices in bfloat16 or wider.
A program may use at most 2 GiB of HBM per device.

```python
import jax
import jax.numpy as jnp
from jax import lax

SEQUENCES = 16
TOKENS = 2048
D = 1024
FF = 2560
LAYERS = 2
NAMES = ("w_gate", "w_up", "w_down")
SHAPES = {"w_gate": (LAYERS, D, FF), "w_up": (LAYERS, D, FF), "w_down": (LAYERS, FF, D)}


def bump(key, n, height):
    away = (jnp.arange(n, dtype=jnp.int32) - jax.random.randint(key, (), 0, n, jnp.int32)) % n
    return jnp.where(away < n // 8, height, 1.0)


def together(key, own, strength):
    shared = jax.random.normal(key, own.shape[1:], jnp.float32)
    return (own + strength * shared) * lax.rsqrt(1 + strength * strength)


def setup_inputs(seed: int = 0, part: int = 0) -> dict:
    kx, kdy, ka, kb, kz, kf, kh, kl, *kw = jax.random.split(jax.random.key(seed), 8 + len(NAMES))
    kx, kdy, ka, kb = (jax.random.fold_in(k, part) for k in (kx, kdy, ka, kb))
    shape = (SEQUENCES, TOKENS, D)
    much_x, much_dy = jax.random.uniform(kz, (2,), jnp.float32, 0.0, 1.0)
    layers = 2.0 ** jax.random.uniform(kl, (LAYERS, 1, 1), jnp.float32, -1.0, 1.0)
    x = together(ka, jax.random.normal(kx, shape, jnp.float32), much_x) * bump(kf, D, 4.0)
    dy = together(kb, jax.random.normal(kdy, shape, jnp.float32), much_dy)
    drawn = {"x": x.astype(jnp.bfloat16), "dy": (dy * (SEQUENCES * TOKENS) ** -0.5).astype(jnp.bfloat16)}
    for key, name in zip(kw, NAMES, strict=True):
        w = jax.random.normal(key, SHAPES[name], jnp.float32) * SHAPES[name][1] ** -0.5
        drawn[name] = (w * {"w_gate": 1.0, "w_up": bump(kh, FF, 4.0), "w_down": layers}[name]).astype(jnp.bfloat16)
    return drawn


def matmul(a, w):
    return jnp.dot(a, w, preferred_element_type=jnp.float32).astype(jnp.bfloat16)


def normed(h):
    wide = h.astype(jnp.float32)
    scale = lax.rsqrt(jnp.mean(wide**2, -1, keepdims=True) + 1e-6)
    return (wide * scale).astype(jnp.bfloat16)


def layer(h, w):
    a = normed(h)
    gate = jnp.dot(a, w["w_gate"], preferred_element_type=jnp.float32)
    up = jnp.dot(a, w["w_up"], preferred_element_type=jnp.float32)
    return h + matmul((jax.nn.silu(gate) * up).astype(jnp.bfloat16), w["w_down"])


def stack(weights, h):
    return lax.scan(lambda h, w: (layer(h, w), None), h, weights)[0]


def reference(x, dy, w_gate, w_up, w_down):
    weights = dict(zip(NAMES, (w_gate, w_up, w_down), strict=True))

    def take(so_far, sequence):
        h, by_y = sequence
        _, back = jax.vjp(stack, weights, h)
        by_weights, by_h = back(by_y)
        return jax.tree.map(lambda total, term: total + term.astype(jnp.float32), so_far, by_weights), by_h

    none_yet = {name: jnp.zeros(w.shape, jnp.float32) for name, w in weights.items()}
    by_weights, by_x = lax.scan(take, none_yet, (x, dy))
    return (by_x, *(by_weights[name].astype(jnp.bfloat16) for name in NAMES))
```

```python
import jax
import jax.numpy as jnp
from jax import lax
from jax.sharding import PartitionSpec as P

F32, BF16 = jnp.float32, jnp.bfloat16


def dot(a, b, dims):
    return lax.dot_general(a, b, (dims, ((), ())), preferred_element_type=F32)


def scale_of(h):
    wide = h.astype(F32)
    return lax.rsqrt(jnp.mean(wide * wide, -1, keepdims=True) + 1e-6)


def normed(h, scale):
    return (h.astype(F32) * scale).astype(BF16)


def solution(mesh):
    def step(x, dy, w_gate, w_up, w_down):
        layers = w_gate.shape[0]
        gather = lambda w: lax.all_gather(w, "dp", axis=0, tiled=True)
        scatter = lambda g: lax.psum_scatter(g, "dp", scatter_dimension=0, tiled=True)
        full = [tuple(gather(w[n]) for w in (w_gate, w_up, w_down)) for n in range(layers)]

        h = x[0]
        saved = []
        for n in range(layers):
            wg, wu, wd = full[n]
            scale = scale_of(h)
            a = normed(h, scale)
            gate = dot(a, wg, ((1,), (0,)))
            up = dot(a, wu, ((1,), (0,)))
            hidden = (jax.nn.silu(gate) * up).astype(BF16)
            saved.append((h, scale, a, gate, up, hidden))
            if n + 1 < layers:
                h = h + dot(hidden, wd, ((1,), (0,))).astype(BF16)

        g = dy[0]
        outs = []
        for n in reversed(range(layers)):
            wg, wu, wd = full[n]
            h, scale, a, gate, up, hidden = saved[n]
            by_wd = dot(hidden, g, ((0,), (0,))).astype(BF16)
            by_hidden = dot(g, wd, ((1,), (1,))).astype(BF16).astype(F32)
            s = jax.nn.sigmoid(gate)
            by_up = (by_hidden * gate * s).astype(BF16)
            by_gate = (by_hidden * up * s * (1 + gate * (1 - s))).astype(BF16)
            by_wg = dot(a, by_gate, ((0,), (0,))).astype(BF16)
            by_wu = dot(a, by_up, ((0,), (0,))).astype(BF16)
            by_a = dot(by_gate, wg, ((1,), (1,))) + dot(by_up, wu, ((1,), (1,)))
            by_a = by_a.astype(BF16).astype(F32)
            wide = h.astype(F32)
            along = jnp.mean(by_a * wide, -1, keepdims=True)
            g = (g.astype(F32) + (scale * (by_a - wide * (scale * scale * along))).astype(BF16).astype(F32)).astype(BF16)
            outs.append((scatter(by_wg), scatter(by_wu), scatter(by_wd)))
        outs = outs[::-1]
        return (g[None], *(jnp.stack([o[i] for o in outs]) for i in range(3)))

    rows, cols = P(("rep", "dp")), P(None, "dp")
    out = P("rep", "dp")
    return jax.shard_map(
        step, mesh=mesh, in_specs=(rows, rows, cols, cols, cols), out_specs=(rows, out, out, out), check_vma=False
    )
```

```python
import functools

import jax
import jax.numpy as jnp
from jax import lax
from jax.experimental import pallas as pl
from jax.experimental.pallas import tpu as pltpu
from jax.sharding import PartitionSpec as P

F32, BF16 = jnp.float32, jnp.bfloat16
S = jax.ShapeDtypeStruct
MESH = pl.DeviceIdType.MESH
ANY = pl.BlockSpec(memory_space=pl.ANY)
DMA = pltpu.SemaphoreType.DMA
CUBE = (4, 2, 1)
LIMIT = 60 << 20


def dot(a, b, ca, cb):
    return lax.dot_general(a, b, (((ca,), (cb,)), ((), ())), preferred_element_type=F32)


def whole(*shape):
    return pl.BlockSpec(shape, lambda i: (0,) * len(shape), pipeline_mode=pl.Buffered(1))


def rows(mt, cols):
    return pl.BlockSpec((mt, cols), lambda i: (i, 0))


def columns(n, nt):
    return pl.BlockSpec((n, nt), lambda i: (0, i))


class Here:
    def __init__(self):
        me, rep = lax.axis_index("dp"), lax.axis_index("rep")
        chip, self.core = me // 2, me % 2
        at = [(chip // d) % 2 for d in CUBE]
        own = [c * d for c, d in zip(at, CUBE)]
        far = [d - o for o, d in zip(own, CUBE)]
        self.other = 1 - self.core
        pick = lambda r: [f if r & d else o for o, f, d in zip(own, far, CUBE)]
        self.chips = [sum(pick(r)[1:], pick(r)[0]) for r in range(8)]
        self.devices = {d: (rep, self.chips[d] * 2 + self.core) for d in CUBE}
        self.devices[0] = (rep, chip * 2 + self.other)

    def meet(self):
        barrier = pltpu.get_barrier_semaphore()
        for d in (*CUBE, 0):
            pl.semaphore_signal(barrier, 1, device_id=self.devices[d], device_id_type=MESH)
        pl.semaphore_wait(barrier, 4)

    def remote(self, src, dst, send, recv, d):
        return pltpu.make_async_remote_copy(
            src_ref=src, dst_ref=dst, send_sem=send, recv_sem=recv, device_id=self.devices[d], device_id_type=MESH
        )


def stripes(cols, first):
    tiles = cols // 128
    cut = [tiles // 3 + (1 if (p + first) % 3 < tiles % 3 else 0) for p in range(3)]
    out, at = [], 0
    for p in range(3):
        out.append((slice(at * 128, (at + cut[p]) * 128), CUBE[p:] + CUBE[:p]))
        at += cut[p]
    return out


class Gather:
    def __init__(self, here, mats, sems):
        self.here = here
        self.mats, (self.send, self.recv, self.dsend, self.drecv, self.local) = mats, sems

    @staticmethod
    def scratch(n):
        return [DMA((n, 3, 7)), DMA((n, 3, 7)), DMA((n, 3, 8)), DMA((n, 3, 8)), DMA((n,))]

    def each(self):
        for m, (src, dst) in enumerate(self.mats):
            for p, (cols, order) in enumerate(stripes(src.shape[-1], m)):
                yield m, p, src, dst, cols, order

    def block(self, item, r, other=False):
        m, p, src, dst, cols, order = item
        here = self.here
        return dst.at[here.chips[r], here.other if other else here.core, :, cols]

    def hop(self, item, j, d):
        m, p, src, dst, cols, order = item
        here = src.at[0, :, cols] if j == 0 else self.block(item, j)
        return self.here.remote(here, self.block(item, j), self.send.at[m, p, (j ^ d) - 1], self.recv.at[m, p, (j ^ d) - 1], d)

    def arrived(self, item, r):
        m, p = item[:2]
        self.here.remote(self.block(item, r), self.block(item, r), self.send.at[m, p, r - 1], self.recv.at[m, p, r - 1], 1).wait_recv()

    def hand(self, item, r):
        m, p, src, dst, cols, order = item
        here = src.at[0, :, cols] if r == 0 else self.block(item, r)
        return self.here.remote(here, self.block(item, r), self.dsend.at[m, p, r], self.drecv.at[m, p, r], 0)

    def stage(self, s):
        items = list(self.each())
        if s == 0:
            for n in range(3):
                for it in items:
                    self.hop(it, 0, it[5][n]).start()
            for it in items:
                self.hand(it, 0).start()
            for m, (src, dst) in enumerate(self.mats):
                pltpu.make_async_copy(src.at[0], dst.at[self.here.chips[0], self.here.core], self.local.at[m]).start()
        if s == 1:
            for it in items:
                d0, d1, d2 = it[5]
                self.arrived(it, d0)
                self.hop(it, d0, d1).start()
                self.hop(it, d0, d2).start()
                self.hand(it, d0).start()
        if s == 2:
            for it in items:
                d0, d1, d2 = it[5]
                for r in (d1, d0 ^ d1):
                    self.arrived(it, r)
                    self.hop(it, r, d2).start()
                    self.hand(it, r).start()
        if s == 3:
            for it in items:
                d0, d1, d2 = it[5]
                for r in (d2, d0 ^ d2, d1 ^ d2, 7):
                    self.arrived(it, r)
                    self.hand(it, r).start()
        if s == 4:
            for it in items:
                m, p = it[:2]
                d0, d1, d2 = it[5]
                for r in range(8):
                    self.here.remote(
                        self.block(it, r, True), self.block(it, r, True), self.dsend.at[m, p, r], self.drecv.at[m, p, r], 0
                    ).wait_recv()
                    self.hand(it, r).wait_send()
                for j, d in ((0, d0), (0, d1), (d0, d1), (0, d2), (d0, d2), (d1, d2), (d0 ^ d1, d2)):
                    self.hop(it, j, d).wait_send()
            for m, (src, dst) in enumerate(self.mats):
                pltpu.make_async_copy(src.at[0], dst.at[self.here.chips[0], self.here.core], self.local.at[m]).wait()


class Scatter:
    PARTS = ((0, 8), (1, 4), (2, 2), (3, 1))

    def __init__(self, here, mats, bufs):
        self.here, self.mats, self.bufs = here, mats, bufs

    @staticmethod
    def scratch(shapes):
        out = []
        for r, c in shapes:
            out += [pltpu.VMEM((n, r, c), BF16) for n in (8, 4, 2, 1)]
            out += [pltpu.VMEM((n, r, c), BF16) for n in (4, 2, 1)]
            out += [DMA((3, 8)), DMA((3, 8)), DMA((3, 7)), DMA((3, 7))]
        return out

    PER = 11

    def each(self):
        for m, (keep, give, out) in enumerate(self.mats):
            b = self.bufs[m * self.PER : (m + 1) * self.PER]
            for p, (cols, order) in enumerate(stripes(keep.shape[-1], m)):
                yield p, keep, give, out, b[:4], b[4:7], b[7:], cols, order

    @staticmethod
    def groups(order):
        d0, d1, d2 = order
        return [[0, d1, d2, d1 ^ d2], [0, d2], [0]]

    def hand(self, it, r):
        p, keep, give, out, inn, leave, sems, cols, order = it
        return self.here.remote(give.at[r, :, cols], inn[0].at[r, :, cols], sems[0].at[p, r], sems[1].at[p, r], 0)

    def hop(self, it, s, n):
        p, keep, give, out, inn, leave, sems, cols, order = it
        k = (0, 4, 6)[s] + n
        return self.here.remote(leave[s].at[n, :, cols], inn[s + 1].at[n, :, cols], sems[2].at[p, k], sems[3].at[p, k], order[s])

    def total(self, it, r, upto):
        p, keep, give, out, inn, leave, sems, cols, order = it
        t = keep[r, :, cols].astype(F32) + inn[0][r, :, cols].astype(F32)
        for s in range(upto):
            t = t + inn[s + 1][self.groups(order)[s].index(r), :, cols].astype(F32)
        return t

    def stage(self, s):
        items = list(self.each())
        if s == 0:
            for first in (True, False):
                for it in items:
                    for r in range(8):
                        if bool(r & it[8][0]) == first:
                            self.hand(it, r).start()
        if s == 1:
            for it in items:
                order, leave, cols = it[8], it[5], it[7]
                for n, r in enumerate(self.groups(order)[0]):
                    self.hand(it, r ^ order[0]).wait_recv()
                    leave[0][n, :, cols] = self.total(it, r ^ order[0], 0).astype(BF16)
                    self.hop(it, 0, n).start()
        if s in (2, 3):
            for it in items:
                order, leave, cols = it[8], it[5], it[7]
                if s == 2:
                    for r in self.groups(order)[0]:
                        self.hand(it, r).wait_recv()
                h = s - 1
                before = self.groups(order)[h - 1]
                for n in range(len(before)):
                    self.hop(it, h - 1, n).wait_recv()
                for n, r in enumerate(self.groups(order)[h]):
                    leave[h][n, :, cols] = self.total(it, r ^ order[h], h).astype(BF16)
                    self.hop(it, h, n).start()
        if s == 4:
            for it in items:
                out, cols = it[3], it[7]
                self.hop(it, 2, 0).wait_recv()
                out[:, cols] = self.total(it, 0, 3).astype(BF16)
            for it in items:
                for r in range(8):
                    self.hand(it, r).wait_send()
                for h, n in ((0, 4), (1, 2), (2, 1)):
                    for k in range(n):
                        self.hop(it, h, k).wait_send()


def at_steps(here, job, steps):
    i = pl.program_id(0)
    for step in sorted(set(steps) - {-1}):

        @pl.when(i == step)
        def _(step=step):
            for s, when in enumerate(steps):
                if when == step:
                    if s == 0:
                        here.meet()
                    job.stage(s)


def call(body, name, grid, ins, outs, shapes, scratch, args, flops, cid=None):
    params = dict(dimension_semantics=("arbitrary",), vmem_limit_bytes=LIMIT)
    if cid is not None:
        params.update(collective_id=cid, has_side_effects=True)
    kw = dict(
        name=name,
        grid=(grid,),
        in_specs=ins,
        out_specs=outs,
        out_shape=shapes,
        scratch_shapes=scratch,
        compiler_params=pltpu.CompilerParams(**params),
        cost_estimate=pl.CostEstimate(flops=flops, bytes_accessed=flops // 500, transcendentals=0),
    )
    if name == "ag_gu0":
        return pl.pallas_call(body, **kw)(*args)
    if name in ("gu0", "gu1"):
        return pl.pallas_call(body, **kw)(*args)
    if name == "down0":
        return pl.pallas_call(body, **kw)(*args)
    if name in ("dwgu1", "dwgu0"):
        return pl.pallas_call(body, **kw)(*args)
    if name == "da1":
        return pl.pallas_call(body, **kw)(*args)
    if name == "da0":
        return pl.pallas_call(body, **kw)(*args)
    return pl.pallas_call(body, **kw)(*args)


def with_job(compute, kind, n_in, n_out, n_scr, mats, steps_of, grid):
    def body(*refs):
        k = mats * (1 if kind is Gather else 2) if kind else 0
        ins, refs = refs[:n_in], refs[n_in:]
        jin, refs = refs[:k], refs[k:]
        outs, refs = refs[:n_out], refs[n_out:]
        jout, refs = refs[:mats], refs[mats:]
        scr, bufs = refs[:n_scr], refs[n_scr:]
        here = Here() if kind else None
        if kind is Gather:
            job = Gather(here, list(zip(jin, jout)), bufs)
        elif kind is Scatter:
            job = Scatter(here, list(zip(jin[::2], jin[1::2], jout)), bufs)
        last = grid - 1
        if kind:
            at_steps(here, job, [s if s < last else -1 for s in steps_of])
        if compute:
            compute(*ins, *outs, *scr)
        if kind:
            at_steps(here, job, [s if s >= last else -1 for s in steps_of])

    return body


def fused(name, grid, compute, ins, outs, shapes, scratch, args, flops, cid=None, gather=None, scatter=None, steps=None):
    ins, outs, shapes, scratch, args = list(ins), list(outs), list(shapes), list(scratch), list(args)
    n_in, n_out, n_scr, kind, mats = len(ins), len(outs), len(scratch), None, 0
    if gather:
        kind, mats = Gather, len(gather)
        for w, layer in gather:
            r, c = w.shape[1:]
            ins.append(pl.BlockSpec((1, r, c), lambda i, layer=layer: (layer, 0, 0), pipeline_mode=pl.Buffered(1)))
            args.append(w)
            outs.append(ANY)
            shapes.append(S((8, 2, r, c), BF16))
        scratch += Gather.scratch(mats)
    if scatter:
        kind, mats = Scatter, len(scatter)
        for keep, give in scatter:
            ins += [whole(*keep.shape), ANY]
            args += [keep, give]
            outs.append(whole(*keep.shape[1:]))
            shapes.append(S(keep.shape[1:], BF16))
        scratch += Scatter.scratch([k.shape[1:] for k, _ in scatter])
    body = with_job(compute, kind, n_in, n_out, n_scr, mats, steps, grid)
    return call(body, name, grid, ins, outs, shapes, scratch, args, flops, cid)


def scale_of(wide):
    return lax.rsqrt(jnp.mean(wide * wide, -1, keepdims=True) + 1e-6)


def gate_up(h, wg, wu, name, **job):
    t, d = h.shape
    ff, nt, mt = wg.shape[1], 256, 512

    def compute(h, wg, wu, gate, up, hidden, a):
        @pl.when(pl.program_id(0) == 0)
        def _():
            for r in range(0, t, 256):
                wide = h[r : r + 256, :].astype(F32)
                a[r : r + 256, :] = (wide * scale_of(wide)).astype(BF16)

        for r in range(0, t, mt):
            at = slice(r, r + mt)
            g, u = dot(a[at, :], wg[...], 1, 0), dot(a[at, :], wu[...], 1, 0)
            gate[at, :], up[at, :] = g, u
            hidden[at, :] = (g * jax.nn.sigmoid(g) * u).astype(BF16)

    tile = columns(t, nt)
    return fused(
        name, ff // nt, compute, [whole(t, d), columns(d, nt), columns(d, nt)], [tile, tile, tile, whole(t, d)],
        [S((t, ff), F32), S((t, ff), F32), S((t, ff), BF16), S((t, d), BF16)], [], [h, wg, wu], 4 * t * d * ff, **job,
    )


def down(hidden, wd, h, name, **job):
    t, ff = hidden.shape
    d, mt = wd.shape[1], 256

    def compute(hidden, wd, h, out):
        m = dot(hidden[...], wd[...], 1, 0).astype(BF16).astype(F32)
        out[...] = (h[...].astype(F32) + m).astype(BF16)

    return fused(
        name, t // mt, compute, [rows(mt, ff), whole(ff, d), rows(mt, d)], [rows(mt, d)], [S((t, d), BF16)], [],
        [hidden, wd, h], 2 * t * d * ff, **job,
    )


def by_hidden(g, wd, gate, up, name, **job):
    t, d = g.shape
    ff, nt, mt = wd.shape[0], 256, 512

    def compute(y, wd, gate, up, by_gate, by_up):
        for r in range(0, t, mt):
            at = slice(r, r + mt)
            b = dot(y[at, :], wd[...], 1, 1).astype(BF16).astype(F32)
            z = gate[at, :]
            s = jax.nn.sigmoid(z)
            by_up[at, :] = (b * z * s).astype(BF16)
            by_gate[at, :] = (b * up[at, :] * s * (1 + z * (1 - s))).astype(BF16)

    tile = columns(t, nt)
    return fused(
        name, ff // nt, compute, [whole(t, d), pl.BlockSpec((nt, d), lambda i: (i, 0)), tile, tile], [tile, tile],
        [S((t, ff), BF16)] * 2, [], [g, wd, gate, up], 2 * t * d * ff, **job,
    )


def split(out, keep, give, tmp, n, r):
    here = Here()
    for chip in range(n):
        for c in range(2):
            tmp[chip, c] = out[(2 * chip + c) * r : (2 * chip + c + 1) * r, :]
    for j in range(n):
        keep[j] = tmp[here.chips[j], here.core]
        give[j] = tmp[here.chips[j], here.other]


def by_gate_up_w(a, by_gate, by_up, name, **job):
    t, d = a.shape
    ff, nt, r = by_gate.shape[1], 512, d // 16

    def compute(a, bg, bu, kg, gg, ku, gu, tmp):
        for b, keep, give in ((bg, kg, gg), (bu, ku, gu)):
            split(dot(a[...], b[...], 0, 0).astype(BF16), keep, give, tmp, 8, r)

    tile = pl.BlockSpec((8, r, nt), lambda i: (0, 0, i))
    return fused(
        name, ff // nt, compute, [whole(t, d), columns(t, nt), columns(t, nt)], [tile] * 4, [S((8, r, ff), BF16)] * 4,
        [pltpu.VMEM((8, 2, r, nt), BF16)], [a, by_gate, by_up], 4 * t * d * ff, **job,
    )


def by_down_w(hidden, g, name, **job):
    t, ff = hidden.shape
    d, nt, r = g.shape[1], 256, ff // 16

    def compute(hidden, g, keep, give, tmp):
        split(dot(hidden[...], g[...], 0, 0).astype(BF16), keep, give, tmp, 8, r)

    tile = pl.BlockSpec((8, r, nt), lambda i: (0, 0, i))
    return fused(
        name, d // nt, compute, [whole(t, ff), columns(t, nt)], [tile] * 2, [S((8, r, d), BF16)] * 2,
        [pltpu.VMEM((8, 2, r, nt), BF16)], [hidden, g], 2 * t * d * ff, **job,
    )


def by_input(by_gate, by_up, wg, wu, h, g, name, **job):
    t, d = h.shape
    ff, mt = by_gate.shape[1], 256

    def compute(bg, bu, wg, wu, h, g, out):
        b = (dot(bg[...], wg[...], 1, 1) + dot(bu[...], wu[...], 1, 1)).astype(BF16).astype(F32)
        wide = h[...].astype(F32)
        s = scale_of(wide)
        along = jnp.mean(b * wide, -1, keepdims=True)
        back = (s * (b - wide * (s * s * along))).astype(BF16).astype(F32)
        out[...] = (g[...].astype(F32) + back).astype(BF16)

    return fused(
        name, t // mt, compute, [rows(mt, ff), rows(mt, ff), whole(d, ff), whole(d, ff), rows(mt, d), rows(mt, d)],
        [rows(mt, d)], [S((t, d), BF16)], [], [by_gate, by_up, wg, wu, h, g], 4 * t * d * ff, **job,
    )


def solution(mesh):
    def step(x, dy, w_gate, w_up, w_down):
        d, ff = w_gate.shape[1] * 16, w_gate.shape[2]
        x, g = x[0], dy[0]
        flat = lambda w, n: w.reshape(n, -1)
        wg0, wu0 = fused("ag_gu0", 1, None, [], [], [], [], [], 1000, 0, gather=[(w_gate, 0), (w_up, 0)], steps=[0] * 5)
        wg0, wu0 = flat(wg0, d), flat(wu0, d)
        gate0, up0, hid0, a0, wd0 = gate_up(x, wg0, wu0, "gu0", cid=1, gather=[(w_down, 0)], steps=[0, 2, 4, 7, 9])
        wd0 = flat(wd0, ff)
        h1, wg1, wu1 = down(hid0, wd0, x, "down0", cid=2, gather=[(w_gate, 1), (w_up, 1)], steps=[0, 3, 6, 7, 7])
        wg1, wu1 = flat(wg1, d), flat(wu1, d)
        gate1, up1, hid1, a1, wd1 = gate_up(h1, wg1, wu1, "gu1", cid=3, gather=[(w_down, 1)], steps=[0, 2, 4, 7, 9])
        wd1 = flat(wd1, ff)

        kd1, gd1 = by_down_w(hid1, g, "dwd1")
        bg1, bu1 = by_hidden(g, wd1, gate1, up1, "dh1")
        kg1, gg1, ku1, gu1, dwd1 = by_gate_up_w(a1, bg1, bu1, "dwgu1", cid=4, scatter=[(kd1, gd1)], steps=[0, 1, 2, 3, 4])
        g, dwg1 = by_input(bg1, bu1, wg1, wu1, h1, g, "da1", cid=5, scatter=[(kg1, gg1)], steps=[0, 1, 4, 5, 7])
        kd0, gd0 = by_down_w(hid0, g, "dwd0")
        bg0, bu0, dwu1 = by_hidden(g, wd0, gate0, up0, "dh0", cid=6, scatter=[(ku1, gu1)], steps=[0, 1, 5, 7, 9])
        kg0, gg0, ku0, gu0, dwd0 = by_gate_up_w(a0, bg0, bu0, "dwgu0", cid=7, scatter=[(kd0, gd0)], steps=[0, 1, 2, 3, 4])
        g, dwg0, dwu0 = by_input(bg0, bu0, wg0, wu0, x, g, "da0", cid=8, scatter=[(kg0, gg0), (ku0, gu0)], steps=[0, 1, 6, 7, 7])
        return g[None], jnp.stack([dwg0, dwg1]), jnp.stack([dwu0, dwu1]), jnp.stack([dwd0, dwd1])

    rows_, cols_, out = P(("rep", "dp")), P(None, "dp"), P("rep", "dp")
    return jax.shard_map(
        step, mesh=mesh, in_specs=(rows_, rows_, cols_, cols_, cols_), out_specs=(rows_, out, out, out), check_vma=False
    )
```

```python
import functools

import jax
import jax.numpy as jnp
from jax import lax
from jax.experimental import pallas as pl
from jax.experimental.pallas import tpu as pltpu
from jax.sharding import PartitionSpec as P

F32, BF16 = jnp.float32, jnp.bfloat16
S = jax.ShapeDtypeStruct
MESH = pl.DeviceIdType.MESH
ANY = pl.BlockSpec(memory_space=pl.ANY)
DMA = pltpu.SemaphoreType.DMA
CUBE = (4, 2, 1)
LIMIT = 67_043_328


def dot(a, b, ca, cb):
    return lax.dot_general(a, b, (((ca,), (cb,)), ((), ())), preferred_element_type=F32)


def whole(*shape):
    return pl.BlockSpec(shape, lambda i: (0,) * len(shape), pipeline_mode=pl.Buffered(1))


def rows(mt, cols):
    return pl.BlockSpec((mt, cols), lambda i: (i, 0))


def columns(n, nt):
    return pl.BlockSpec((n, nt), lambda i: (0, i))


class Here:
    def __init__(self):
        me, rep = lax.axis_index("dp"), lax.axis_index("rep")
        chip, self.core = me // 2, me % 2
        self.at = at = [(chip // d) % 2 for d in CUBE]
        own = [c * d for c, d in zip(at, CUBE)]
        far = [d - o for o, d in zip(own, CUBE)]
        self.other = 1 - self.core
        pick = lambda r: [f if r & d else o for o, f, d in zip(own, far, CUBE)]
        self.chips = [sum(pick(r)[1:], pick(r)[0]) for r in range(8)]
        self.devices = {d: (rep, self.chips[d] * 2 + self.core) for d in CUBE}
        self.devices[0] = (rep, chip * 2 + self.other)

    def meet(self):
        barrier = pltpu.get_barrier_semaphore()
        for d in (*CUBE, 0):
            pl.semaphore_signal(barrier, 1, device_id=self.devices[d], device_id_type=MESH)
        pl.semaphore_wait(barrier, 4)

    def remote(self, src, dst, send, recv, d):
        return pltpu.make_async_remote_copy(
            src_ref=src, dst_ref=dst, send_sem=send, recv_sem=recv, device_id=self.devices[d], device_id_type=MESH
        )


def stripes(cols, first):
    tiles = cols // 128
    cut = [tiles // 3 + (1 if (p + first) % 3 < tiles % 3 else 0) for p in range(3)]
    out, at = [], 0
    for p in range(3):
        out.append((slice(at * 128, (at + cut[p]) * 128), CUBE[p:] + CUBE[:p]))
        at += cut[p]
    return out


class Gather:
    def __init__(self, here, mats, sems):
        self.here = here
        self.mats, (self.send, self.recv, self.dsend, self.drecv, self.local) = mats, sems

    @staticmethod
    def scratch(n):
        return [DMA((n, 3, 7)), DMA((n, 3, 7)), DMA((n, 3, 8)), DMA((n, 3, 8)), DMA((n,))]

    def each(self):
        for m, (src, dst) in enumerate(self.mats):
            for p, (cols, order) in enumerate(stripes(src.shape[-1], m)):
                yield m, p, src, dst, cols, order

    def block(self, item, r, other=False):
        m, p, src, dst, cols, order = item
        here = self.here
        return dst.at[here.chips[r], here.other if other else here.core, :, cols]

    def hop(self, item, j, d):
        m, p, src, dst, cols, order = item
        here = src.at[0, :, cols] if j == 0 else self.block(item, j)
        return self.here.remote(here, self.block(item, j), self.send.at[m, p, (j ^ d) - 1], self.recv.at[m, p, (j ^ d) - 1], d)

    def arrived(self, item, r):
        m, p = item[:2]
        self.here.remote(self.block(item, r), self.block(item, r), self.send.at[m, p, r - 1], self.recv.at[m, p, r - 1], 1).wait_recv()

    def hand(self, item, r):
        m, p, src, dst, cols, order = item
        here = src.at[0, :, cols] if r == 0 else self.block(item, r)
        return self.here.remote(here, self.block(item, r), self.dsend.at[m, p, r], self.drecv.at[m, p, r], 0)

    def stage(self, s):
        items = list(self.each())
        if s == 0:
            for n in range(3):
                for it in items:
                    self.hop(it, 0, it[5][n]).start()
            for it in items:
                self.hand(it, 0).start()
            for m, (src, dst) in enumerate(self.mats):
                pltpu.make_async_copy(src.at[0], dst.at[self.here.chips[0], self.here.core], self.local.at[m]).start()
        if s == 1:
            for it in items:
                d0, d1, d2 = it[5]
                self.arrived(it, d0)
                self.hop(it, d0, d1).start()
                self.hop(it, d0, d2).start()
                self.hand(it, d0).start()
        if s == 2:
            for it in items:
                d0, d1, d2 = it[5]
                for r in (d1, d0 ^ d1):
                    self.arrived(it, r)
                    self.hop(it, r, d2).start()
                    self.hand(it, r).start()
        if s == 3:
            for it in items:
                d0, d1, d2 = it[5]
                for r in (d2, d0 ^ d2, d1 ^ d2, 7):
                    self.arrived(it, r)
                    self.hand(it, r).start()
        if s == 4:
            for it in items:
                m, p = it[:2]
                d0, d1, d2 = it[5]
                for r in range(8):
                    self.here.remote(
                        self.block(it, r, True), self.block(it, r, True), self.dsend.at[m, p, r], self.drecv.at[m, p, r], 0
                    ).wait_recv()
                    self.hand(it, r).wait_send()
                for j, d in ((0, d0), (0, d1), (d0, d1), (0, d2), (d0, d2), (d1, d2), (d0 ^ d1, d2)):
                    self.hop(it, j, d).wait_send()
            for m, (src, dst) in enumerate(self.mats):
                pltpu.make_async_copy(src.at[0], dst.at[self.here.chips[0], self.here.core], self.local.at[m]).wait()


class Scatter:
    PARTS = ((0, 8), (1, 4), (2, 2), (3, 1))

    def __init__(self, here, mats, bufs):
        self.here, self.mats, self.bufs = here, mats, bufs

    @staticmethod
    def scratch(shapes):
        out = []
        for r, c in shapes:
            out += [pltpu.VMEM((n, r, c), BF16) for n in (8, 4, 2, 1)]
            out += [pltpu.VMEM((n, r, c), BF16) for n in (4, 2, 1)]
            out += [DMA((3, 8)), DMA((3, 8)), DMA((3, 7)), DMA((3, 7))]
        return out

    PER = 11

    def each(self):
        for m, (keep, give, out) in enumerate(self.mats):
            b = self.bufs[m * self.PER : (m + 1) * self.PER]
            for p, (cols, order) in enumerate(stripes(keep.shape[-1], m)):
                yield p, keep, give, out, b[:4], b[4:7], b[7:], cols, order

    @staticmethod
    def groups(order):
        d0, d1, d2 = order
        return [[0, d1, d2, d1 ^ d2], [0, d2], [0]]

    def hand(self, it, r):
        p, keep, give, out, inn, leave, sems, cols, order = it
        return self.here.remote(give.at[r, :, cols], inn[0].at[r, :, cols], sems[0].at[p, r], sems[1].at[p, r], 0)

    def hop(self, it, s, n):
        p, keep, give, out, inn, leave, sems, cols, order = it
        k = (0, 4, 6)[s] + n
        return self.here.remote(leave[s].at[n, :, cols], inn[s + 1].at[n, :, cols], sems[2].at[p, k], sems[3].at[p, k], order[s])

    def total(self, it, r, upto):
        p, keep, give, out, inn, leave, sems, cols, order = it
        t = keep[r, :, cols].astype(F32) + inn[0][r, :, cols].astype(F32)
        for s in range(upto):
            t = t + inn[s + 1][self.groups(order)[s].index(r), :, cols].astype(F32)
        return t

    def stage(self, s):
        items = list(self.each())
        if s == 0:
            for first in (True, False):
                for it in items:
                    for r in range(8):
                        if bool(r & it[8][0]) == first:
                            self.hand(it, r).start()
        if s == 1:
            for it in items:
                order, leave, cols = it[8], it[5], it[7]
                for n, r in enumerate(self.groups(order)[0]):
                    self.hand(it, r ^ order[0]).wait_recv()
                    leave[0][n, :, cols] = self.total(it, r ^ order[0], 0).astype(BF16)
                    self.hop(it, 0, n).start()
        if s in (2, 3):
            for it in items:
                order, leave, cols = it[8], it[5], it[7]
                if s == 2:
                    for r in self.groups(order)[0]:
                        self.hand(it, r).wait_recv()
                h = s - 1
                before = self.groups(order)[h - 1]
                for n in range(len(before)):
                    self.hop(it, h - 1, n).wait_recv()
                for n, r in enumerate(self.groups(order)[h]):
                    leave[h][n, :, cols] = self.total(it, r ^ order[h], h).astype(BF16)
                    self.hop(it, h, n).start()
        if s == 4:
            for it in items:
                out, cols = it[3], it[7]
                self.hop(it, 2, 0).wait_recv()
                out[:, cols] = self.total(it, 0, 3).astype(BF16)
            for it in items:
                for r in range(8):
                    self.hand(it, r).wait_send()
                for h, n in ((0, 4), (1, 2), (2, 1)):
                    for k in range(n):
                        self.hop(it, h, k).wait_send()


def at_steps(here, job, steps, meet=True):
    i = pl.program_id(0)
    for step in sorted(set(steps) - {-1}):

        @pl.when(i == step)
        def _(step=step):
            for s, when in enumerate(steps):
                if when == step:
                    if s == 0 and meet:
                        here.meet()
                    job.stage(s)


def call(body, name, grid, ins, outs, shapes, scratch, args, flops, cid=None):
    params = dict(dimension_semantics=("arbitrary",), vmem_limit_bytes=LIMIT)
    if cid is not None:
        params.update(collective_id=cid, has_side_effects=True)
    kw = dict(
        name=name,
        grid=(grid,),
        in_specs=ins,
        out_specs=outs,
        out_shape=shapes,
        scratch_shapes=scratch,
        compiler_params=pltpu.CompilerParams(**params),
        cost_estimate=pl.CostEstimate(flops=flops, bytes_accessed=flops // 500, transcendentals=0),
    )
    return pl.pallas_call(body, **kw)(*args)


def with_job(compute, kind, n_in, n_out, n_scr, mats, steps_of, grid):
    def body(*refs):
        k = mats * (1 if kind is Gather else 2) if kind else 0
        ins, refs = refs[:n_in], refs[n_in:]
        jin, refs = refs[:k], refs[k:]
        outs, refs = refs[:n_out], refs[n_out:]
        jout, refs = refs[:mats], refs[mats:]
        scr, bufs = refs[:n_scr], refs[n_scr:]
        here = Here() if kind else None
        if kind is Gather:
            job = Gather(here, list(zip(jin, jout)), bufs)
        elif kind is Scatter:
            job = Scatter(here, list(zip(jin[::2], jin[1::2], jout)), bufs)
        last = grid - 1
        if kind:
            at_steps(here, job, [s if s < last else -1 for s in steps_of])
        if compute:
            compute(*ins, *outs, *scr)
        if kind:
            at_steps(here, job, [s if s >= last else -1 for s in steps_of])

    return body


def fused(name, grid, compute, ins, outs, shapes, scratch, args, flops, cid=None, gather=None, scatter=None, steps=None):
    ins, outs, shapes, scratch, args = list(ins), list(outs), list(shapes), list(scratch), list(args)
    n_in, n_out, n_scr, kind, mats = len(ins), len(outs), len(scratch), None, 0
    if gather:
        kind, mats = Gather, len(gather)
        for w, layer in gather:
            r, c = w.shape[1:]
            ins.append(pl.BlockSpec((1, r, c), lambda i, layer=layer: (layer, 0, 0), pipeline_mode=pl.Buffered(1)))
            args.append(w)
            outs.append(ANY)
            shapes.append(S((8, 2, r, c), BF16))
        scratch += Gather.scratch(mats)
    if scatter:
        kind, mats = Scatter, len(scatter)
        for keep, give in scatter:
            ins += [whole(*keep.shape), ANY]
            args += [keep, give]
            outs.append(whole(*keep.shape[1:]))
            shapes.append(S(keep.shape[1:], BF16))
        scratch += Scatter.scratch([k.shape[1:] for k, _ in scatter])
    body = with_job(compute, kind, n_in, n_out, n_scr, mats, steps, grid)
    return call(body, name, grid, ins, outs, shapes, scratch, args, flops, cid)


def scale_of(wide):
    return lax.rsqrt(jnp.mean(wide * wide, -1, keepdims=True) + 1e-6)


def norm_into(h, a):
    for r in range(0, h.shape[0], 256):
        wide = h[r : r + 256, :].astype(F32)
        a[r : r + 256, :] = (wide * scale_of(wide)).astype(BF16)


def gate_up(h, wg, wu, name, **job):
    t, d = h.shape
    ff, nt, mt = wg.shape[1], 256, 512

    def compute(h, wg, wu, by_g, by_u, hidden, a):
        @pl.when(pl.program_id(0) == 0)
        def _():
            norm_into(h, a)

        for r in range(0, t, mt):
            at = slice(r, r + mt)
            g, u = dot(a[at, :], wg[...], 1, 0), dot(a[at, :], wu[...], 1, 0)
            hid, by_g[at, :], by_u[at, :] = activation(g, u)
            hidden[at, :] = hid.astype(BF16)

    tile = columns(t, nt)
    return fused(
        name, ff // nt, compute, [whole(t, d), columns(d, nt), columns(d, nt)], [tile, tile, tile, whole(t, d)],
        [S((t, ff), F32), S((t, ff), F32), S((t, ff), BF16), S((t, d), BF16)], [], [h, wg, wu], 4 * t * d * ff, **job,
    )


def down(hidden, wd, h, name, **job):
    t, ff = hidden.shape
    d, mt = wd.shape[1], 256

    def compute(hidden, wd, h, out):
        m = dot(hidden[...], wd[...], 1, 0).astype(BF16).astype(F32)
        out[...] = (h[...].astype(F32) + m).astype(BF16)

    return fused(
        name, t // mt, compute, [rows(mt, ff), whole(ff, d), rows(mt, d)], [rows(mt, d)], [S((t, d), BF16)], [],
        [hidden, wd, h], 2 * t * d * ff, **job,
    )


def down_grad(here, i, steps, w, keep, give, tmp, sems):
    pairs, r = tmp.shape[1], tmp.shape[3]

    def move(step, act):
        for pair in range(pairs):
            chip = step * pairs + pair
            bits = [(chip // e) % 2 for e in CUBE]
            a, b, c = [(v + o - 2 * v * o) * e for v, o, e in zip(bits, here.at, CUBE)]
            for n, (to, core) in enumerate(((keep, here.core), (give, here.other))):
                copy = pltpu.make_async_copy(tmp.at[step % 2, pair, core], to.at[a + b + c], sems.at[step % 2, pair, n])
                getattr(copy, act)()

    @pl.when(i >= 2)
    def _():
        move(i - 2, "wait")

    for k in range(2 * pairs):
        tmp[i % 2, k // 2, k % 2] = w[k * r : (k + 1) * r, :]
    move(i, "start")

    @pl.when(i == steps - 1)
    def _():
        move(i - 1, "wait")
        move(i, "wait")


def activation(g, u):
    s = 0.5 * jnp.tanh(0.5 * g) + 0.5
    silu = g * s
    return silu * u, u * (s + silu * (1 - s)), silu


def last_layer(h, wg, wu, wd, g, name, **job):
    t, d = h.shape
    ff, nt, mt = wd.shape[0], 640, 512
    r, steps = ff // 16, ff // nt
    each = nt // r

    def compute(h, wg, wu, wd, y, bgu, a, keep, give, hidden, tmp, sems):
        here, i = Here(), pl.program_id(0)

        @pl.when(i == 0)
        def _():
            norm_into(h, a)

        for at in (slice(r0, r0 + mt) for r0 in range(0, t, mt)):
            hid, mg, mu = activation(dot(a[at, :], wg[...], 1, 0), dot(a[at, :], wu[...], 1, 0))
            hidden[at, :] = hid.astype(BF16)
            b = dot(y[at, :], wd[...], 1, 1).astype(BF16).astype(F32)
            bgu[0, at, :] = (b * mg).astype(BF16)
            bgu[1, at, :] = (b * mu).astype(BF16)
        down_grad(here, i, steps, dot(hidden[...], y[...], 0, 0).astype(BF16), keep, give, tmp, sems)

    return fused(
        name, steps, compute,
        [whole(t, d), columns(d, nt), columns(d, nt), pl.BlockSpec((nt, d), lambda i: (i, 0)), whole(t, d)],
        [pl.BlockSpec((2, t, nt), lambda i: (0, 0, i)), whole(t, d), ANY, ANY],
        [S((2, t, ff), BF16), S((t, d), BF16)] + [S((8, r, d), BF16)] * 2,
        [pltpu.VMEM((t, nt), BF16), pltpu.VMEM((2, each // 2, 2, r, d), BF16), DMA((2, each // 2, 2))],
        [h, wg, wu, wd, g], 8 * t * d * ff, **job,
    )


def by_hidden(g, wd, by_g, by_u, hidden, name, **job):
    t, d = g.shape
    ff, nt, mt = wd.shape[0], 640, 512
    r, steps = ff // 16, ff // nt
    each = nt // r

    def compute(y, wd, mg, mu, hidden, bgu, keep, give, tmp, sems):
        here, i = Here(), pl.program_id(0)

        for at in (slice(r0, r0 + mt) for r0 in range(0, t, mt)):
            b = dot(y[at, :], wd[...], 1, 1).astype(BF16).astype(F32)
            bgu[0, at, :] = (b * mg[at, :]).astype(BF16)
            bgu[1, at, :] = (b * mu[at, :]).astype(BF16)
        down_grad(here, i, steps, dot(hidden[...], y[...], 0, 0).astype(BF16), keep, give, tmp, sems)

    tile, pair = columns(t, nt), pl.BlockSpec((2, t, nt), lambda i: (0, 0, i))
    return fused(
        name, steps, compute, [whole(t, d), pl.BlockSpec((nt, d), lambda i: (i, 0)), tile, tile, tile], [pair, ANY, ANY],
        [S((2, t, ff), BF16)] + [S((8, r, d), BF16)] * 2, [pltpu.VMEM((2, each // 2, 2, r, d), BF16), DMA((2, each // 2, 2))],
        [g, wd, by_g, by_u, hidden], 4 * t * d * ff, **job,
    )


def layer_end(a, bgu, wg, wu, h, g, keep, give, name, cid, plans):
    t, d = h.shape
    ff, nt, mt, r = bgu.shape[2], 512, 256, d // 16
    n = ff // nt
    first, second = 2 * n, t // mt
    last = first + second - 1

    def body(a, cols, both, wg, wu, h, g, keep, give, out, dwd, dwg, dwu, kgu, ggu, tmp, *bufs):
        i, here, per = pl.program_id(0), Here(), Scatter.PER
        jobs = [
            Scatter(here, [mats], bufs[k * per : (k + 1) * per])
            for k, mats in enumerate(((keep, give, dwd), (kgu.at[0], ggu.at[0], dwg), (kgu.at[1], ggu.at[1], dwu)))
        ]

        @pl.when(i == 0)
        def _():
            here.meet()

        for job, plan in zip(jobs, plans):
            at_steps(here, job, [s if s <= last else -1 for s in plan], False)

        @pl.when(i < first)
        def _():
            w = dot(a[...], cols[0], 0, 0).astype(BF16)
            for c in range(16):
                tmp[c // 2, c % 2] = w[c * r : (c + 1) * r, :]
            at = pl.ds(pl.multiple_of((i % n) * nt, nt), nt)
            for j in range(8):
                kgu[i // n, j, :, at] = tmp[here.chips[j], here.core]
                ggu[i // n, j, :, at] = tmp[here.chips[j], here.other]

        @pl.when(i >= first)
        def _():
            b = (dot(both[0], wg[...], 1, 1) + dot(both[1], wu[...], 1, 1)).astype(BF16).astype(F32)
            wide = h[...].astype(F32)
            s = scale_of(wide)
            along = jnp.mean(b * wide, -1, keepdims=True)
            back = (s * (b - wide * (s * s * along))).astype(BF16).astype(F32)
            out[...] = (g[...].astype(F32) + back).astype(BF16)

        for s in range(5):
            for job, plan in zip(jobs, plans):
                if plan[s] > last:
                    at_steps(here, job, [last if q == s else -1 for q in range(5)], False)

    late = lambda i: jnp.maximum(i - first, 0)
    row = pl.BlockSpec((mt, d), lambda i: (late(i), 0))
    early = lambda i: jnp.minimum(i, first - 1)
    shapes = [keep.shape[1:], (r, ff), (r, ff)]
    return call(
        body, name, first + second,
        [
            whole(t, d),
            pl.BlockSpec((1, t, nt), lambda i: (early(i) // n, 0, early(i) % n)),
            pl.BlockSpec((2, mt, ff), lambda i: (0, late(i), 0)),
            whole(d, ff), whole(d, ff), row, row, whole(*keep.shape), ANY,
        ],
        [row] + [whole(*s) for s in shapes],
        [S((t, d), BF16)] + [S(s, BF16) for s in shapes],
        [pltpu.VMEM((2, 8, r, ff), BF16), pltpu.VMEM((2, 8, r, ff), BF16), pltpu.VMEM((8, 2, r, nt), BF16)] + Scatter.scratch(shapes),
        [a, bgu, bgu, wg, wu, h, g, keep, give], 8 * t * d * ff, cid,
    )


def solution(mesh):
    def step(x, dy, w_gate, w_up, w_down):
        d, ff = w_gate.shape[1] * 16, w_gate.shape[2]
        x, g = x[0], dy[0]
        flat = lambda w, n: w.reshape(n, -1)
        wg0, wu0 = fused("ag_gu0", 1, None, [], [], [], [], [], 1000, 0, gather=[(w_gate, 0), (w_up, 0)], steps=[0] * 5)
        wg0, wu0 = flat(wg0, d), flat(wu0, d)
        mg0, mu0, hid0, a0, wd0, wd1 = gate_up(x, wg0, wu0, "gu0", cid=1, gather=[(w_down, 0), (w_down, 1)], steps=[0, 3, 5, 8, 9])
        wd0, wd1 = flat(wd0, ff), flat(wd1, ff)
        h1, wg1, wu1 = down(hid0, wd0, x, "down0", cid=2, gather=[(w_gate, 1), (w_up, 1)], steps=[0, 3, 6, 7, 7])
        wg1, wu1 = flat(wg1, d), flat(wu1, d)

        bgu1, a1, kd1, gd1 = last_layer(h1, wg1, wu1, wd1, g, "last")
        plans = [[0, 2, 6, 9, 10], [5, 7, 12, 14, 16], [10, 12, 17, 99, 99]]
        g, dwd1, dwg1, dwu1 = layer_end(a1, bgu1, wg1, wu1, h1, g, kd1, gd1, "end1", 3, plans)
        bgu0, kd0, gd0 = by_hidden(g, wd0, mg0, mu0, hid0, "dh0")
        g, dwd0, dwg0, dwu0 = layer_end(a0, bgu0, wg0, wu0, x, g, kd0, gd0, "end0", 4, plans)
        return g[None], jnp.stack([dwg0, dwg1]), jnp.stack([dwu0, dwu1]), jnp.stack([dwd0, dwd1])

    rows_, cols_, out = P(("rep", "dp")), P(None, "dp"), P("rep", "dp")
    return jax.shard_map(
        step, mesh=mesh, in_specs=(rows_, rows_, cols_, cols_, cols_), out_specs=(rows_, out, out, out), check_vma=False
    )
```

```python
import functools

import jax
import jax.numpy as jnp
from jax import lax
from jax.experimental import pallas as pl
from jax.experimental.pallas import tpu as pltpu
from jax.sharding import PartitionSpec as P

F32, BF16 = jnp.float32, jnp.bfloat16
S = jax.ShapeDtypeStruct
MESH = pl.DeviceIdType.MESH
ANY = pl.BlockSpec(memory_space=pl.ANY)
DMA = pltpu.SemaphoreType.DMA
CUBE = (4, 2, 1)
LIMIT = 67_043_328


def dot(a, b, ca, cb):
    return lax.dot_general(a, b, (((ca,), (cb,)), ((), ())), preferred_element_type=F32)


def whole(*shape):
    return pl.BlockSpec(shape, lambda i: (0,) * len(shape), pipeline_mode=pl.Buffered(1))


def rows(mt, cols):
    return pl.BlockSpec((mt, cols), lambda i: (i, 0))


def columns(n, nt):
    return pl.BlockSpec((n, nt), lambda i: (0, i))


class Here:
    def __init__(self):
        me, rep = lax.axis_index("dp"), lax.axis_index("rep")
        chip, self.core = me // 2, me % 2
        self.at = at = [(chip // d) % 2 for d in CUBE]
        own = [c * d for c, d in zip(at, CUBE)]
        far = [d - o for o, d in zip(own, CUBE)]
        self.other = 1 - self.core
        pick = lambda r: [f if r & d else o for o, f, d in zip(own, far, CUBE)]
        self.chips = [sum(pick(r)[1:], pick(r)[0]) for r in range(8)]
        self.devices = {d: (rep, self.chips[d] * 2 + self.core) for d in CUBE}
        self.devices[0] = (rep, chip * 2 + self.other)

    def meet(self):
        barrier = pltpu.get_barrier_semaphore()
        for d in (*CUBE, 0):
            pl.semaphore_signal(barrier, 1, device_id=self.devices[d], device_id_type=MESH)
        pl.semaphore_wait(barrier, 4)

    def remote(self, src, dst, send, recv, d):
        return pltpu.make_async_remote_copy(
            src_ref=src, dst_ref=dst, send_sem=send, recv_sem=recv, device_id=self.devices[d], device_id_type=MESH
        )


def stripes(cols, first):
    tiles = cols // 128
    cut = [tiles // 3 + (1 if (p + first) % 3 < tiles % 3 else 0) for p in range(3)]
    out, at = [], 0
    for p in range(3):
        out.append((slice(at * 128, (at + cut[p]) * 128), CUBE[p:] + CUBE[:p]))
        at += cut[p]
    return out


class Gather:
    def __init__(self, here, mats, sems):
        self.here = here
        self.mats, (self.send, self.recv, self.dsend, self.drecv, self.local) = mats, sems

    @staticmethod
    def scratch(n):
        return [DMA((n, 3, 7)), DMA((n, 3, 7)), DMA((n, 3, 8)), DMA((n, 3, 8)), DMA((n,))]

    def each(self):
        for m, (src, dst) in enumerate(self.mats):
            for p, (cols, order) in enumerate(stripes(src.shape[-1], m)):
                yield m, p, src, dst, cols, order

    def block(self, item, r, other=False):
        m, p, src, dst, cols, order = item
        here = self.here
        return dst.at[here.chips[r], here.other if other else here.core, :, cols]

    def hop(self, item, j, d):
        m, p, src, dst, cols, order = item
        here = src.at[0, :, cols] if j == 0 else self.block(item, j)
        return self.here.remote(here, self.block(item, j), self.send.at[m, p, (j ^ d) - 1], self.recv.at[m, p, (j ^ d) - 1], d)

    def arrived(self, item, r):
        m, p = item[:2]
        self.here.remote(self.block(item, r), self.block(item, r), self.send.at[m, p, r - 1], self.recv.at[m, p, r - 1], 1).wait_recv()

    def hand(self, item, r):
        m, p, src, dst, cols, order = item
        here = src.at[0, :, cols] if r == 0 else self.block(item, r)
        return self.here.remote(here, self.block(item, r), self.dsend.at[m, p, r], self.drecv.at[m, p, r], 0)

    def stage(self, s):
        items = list(self.each())
        if s == 0:
            for n in range(3):
                for it in items:
                    self.hop(it, 0, it[5][n]).start()
            for it in items:
                self.hand(it, 0).start()
            for m, (src, dst) in enumerate(self.mats):
                pltpu.make_async_copy(src.at[0], dst.at[self.here.chips[0], self.here.core], self.local.at[m]).start()
        if s == 1:
            for it in items:
                d0, d1, d2 = it[5]
                self.arrived(it, d0)
                self.hop(it, d0, d1).start()
                self.hop(it, d0, d2).start()
                self.hand(it, d0).start()
        if s == 2:
            for it in items:
                d0, d1, d2 = it[5]
                for r in (d1, d0 ^ d1):
                    self.arrived(it, r)
                    self.hop(it, r, d2).start()
                    self.hand(it, r).start()
        if s == 3:
            for it in items:
                d0, d1, d2 = it[5]
                for r in (d2, d0 ^ d2, d1 ^ d2, 7):
                    self.arrived(it, r)
                    self.hand(it, r).start()
        if s == 4:
            for it in items:
                m, p = it[:2]
                d0, d1, d2 = it[5]
                for r in range(8):
                    self.here.remote(
                        self.block(it, r, True), self.block(it, r, True), self.dsend.at[m, p, r], self.drecv.at[m, p, r], 0
                    ).wait_recv()
                    self.hand(it, r).wait_send()
                for j, d in ((0, d0), (0, d1), (d0, d1), (0, d2), (d0, d2), (d1, d2), (d0 ^ d1, d2)):
                    self.hop(it, j, d).wait_send()
            for m, (src, dst) in enumerate(self.mats):
                pltpu.make_async_copy(src.at[0], dst.at[self.here.chips[0], self.here.core], self.local.at[m]).wait()


class Scatter:
    def __init__(self, here, mats, bufs):
        self.here, self.mats, self.bufs = here, mats, bufs

    @staticmethod
    def scratch(shapes):
        out = []
        for r, c in shapes:
            out += [pltpu.VMEM((n, r, c), BF16) for n in (8, 4, 2, 1)]
            out += [pltpu.VMEM((n, r, c), BF16) for n in (4, 2, 1)]
            out += [DMA((3, 8)), DMA((3, 8)), DMA((3, 7)), DMA((3, 7))]
        return out

    PER = 11

    def each(self):
        for m, (keep, give, out) in enumerate(self.mats):
            b = self.bufs[m * self.PER : (m + 1) * self.PER]
            for p, (cols, order) in enumerate(stripes(keep.shape[-1], m)):
                yield p, keep, give, out, b[:4], b[4:7], b[7:], cols, order

    @staticmethod
    def groups(order):
        d0, d1, d2 = order
        return [[d1, d1 ^ d2, d2, 0], [d2, 0], [0]]

    def hand(self, it, r):
        p, keep, give, out, inn, leave, sems, cols, order = it
        return self.here.remote(give(r).at[:, cols], inn[0].at[r, :, cols], sems[0].at[p, r], sems[1].at[p, r], 0)

    def hop(self, it, s, n):
        p, keep, give, out, inn, leave, sems, cols, order = it
        k = (0, 4, 6)[s] + n
        return self.here.remote(leave[s].at[n, :, cols], inn[s + 1].at[n, :, cols], sems[2].at[p, k], sems[3].at[p, k], order[s])

    def total(self, it, r, upto):
        p, keep, give, out, inn, leave, sems, cols, order = it
        t = keep[r, :, cols].astype(F32) + inn[0][r, :, cols].astype(F32)
        for s in range(upto):
            t = t + inn[s + 1][self.groups(order)[s].index(r), :, cols].astype(F32)
        return t

    def stage(self, s):
        items = list(self.each())
        if s == 0:
            for first in (True, False):
                for it in items:
                    for r in range(8):
                        if bool(r & it[8][0]) == first:
                            self.hand(it, r).start()
            return
        for it in items:
            out, leave, cols, order = it[3], it[5], it[7], it[8]
            groups, h = self.groups(order), s - 1
            going = [r ^ order[h] for r in groups[h]] if s < 4 else [0]
            for n, r in enumerate(going):
                self.hand(it, r).wait_recv()
                for k in range(h):
                    self.hop(it, k, groups[k].index(r)).wait_recv()
                t = self.total(it, r, h).astype(BF16)
                if s < 4:
                    leave[h][n, :, cols] = t
                    self.hop(it, h, n).start()
                else:
                    out[:, cols] = t
        if s == 4:
            for it in items:
                for r in range(8):
                    self.hand(it, r).wait_send()
                for h, n in ((0, 4), (1, 2), (2, 1)):
                    for k in range(n):
                        self.hop(it, h, k).wait_send()


def at_steps(here, job, steps, meet=True):
    i = pl.program_id(0)
    for step in sorted(set(steps) - {-1}):

        @pl.when(i == step)
        def _(step=step):
            for s, when in enumerate(steps):
                if when == step:
                    if s == 0 and meet:
                        here.meet()
                    job.stage(s)


def call(body, name, grid, ins, outs, shapes, scratch, args, flops, cid=None):
    params = dict(dimension_semantics=("arbitrary",), vmem_limit_bytes=LIMIT)
    if cid is not None:
        params.update(collective_id=cid, has_side_effects=True)
    kw = dict(
        name=name,
        grid=(grid,),
        in_specs=ins,
        out_specs=outs,
        out_shape=shapes,
        scratch_shapes=scratch,
        compiler_params=pltpu.CompilerParams(**params),
        cost_estimate=pl.CostEstimate(flops=flops, bytes_accessed=flops // 500, transcendentals=0),
    )
    return pl.pallas_call(body, **kw)(*args)


def with_job(compute, kind, n_in, n_out, n_scr, mats, steps_of, grid):
    def body(*refs):
        k = mats * (1 if kind is Gather else 2) if kind else 0
        ins, refs = refs[:n_in], refs[n_in:]
        jin, refs = refs[:k], refs[k:]
        outs, refs = refs[:n_out], refs[n_out:]
        jout, refs = refs[:mats], refs[mats:]
        scr, bufs = refs[:n_scr], refs[n_scr:]
        here = Here() if kind else None
        if kind is Gather:
            job = Gather(here, list(zip(jin, jout)), bufs)
        elif kind is Scatter:
            job = Scatter(here, [(k, lambda r, g=g: g.at[r], o) for k, g, o in zip(jin[::2], jin[1::2], jout)], bufs)
        last = grid - 1
        if kind:
            at_steps(here, job, [s if s < last or not n else -1 for n, s in enumerate(steps_of)])
        if compute:
            compute(*ins, *outs, *scr)
        if kind:
            at_steps(here, job, [s if s >= last and n else -1 for n, s in enumerate(steps_of)])

    return body


def fused(name, grid, compute, ins, outs, shapes, scratch, args, flops, cid=None, gather=None, scatter=None, steps=None):
    ins, outs, shapes, scratch, args = list(ins), list(outs), list(shapes), list(scratch), list(args)
    n_in, n_out, n_scr, kind, mats = len(ins), len(outs), len(scratch), None, 0
    if gather:
        kind, mats = Gather, len(gather)
        for w, layer in gather:
            r, c = w.shape[1:]
            ins.append(pl.BlockSpec((1, r, c), lambda i, layer=layer: (layer, 0, 0), pipeline_mode=pl.Buffered(1)))
            args.append(w)
            outs.append(ANY)
            shapes.append(S((8, 2, r, c), BF16))
        scratch += Gather.scratch(mats)
    if scatter:
        kind, mats = Scatter, len(scatter)
        for keep, give in scatter:
            ins += [whole(*keep.shape), ANY]
            args += [keep, give]
            outs.append(whole(*keep.shape[1:]))
            shapes.append(S(keep.shape[1:], BF16))
        scratch += Scatter.scratch([k.shape[1:] for k, _ in scatter])
    body = with_job(compute, kind, n_in, n_out, n_scr, mats, steps, grid)
    return call(body, name, grid, ins, outs, shapes, scratch, args, flops, cid)


def scale_of(wide):
    return lax.rsqrt(jnp.mean(wide * wide, -1, keepdims=True) + 1e-6)


def norm_into(h, a):
    for r in range(0, h.shape[0], 256):
        wide = h[r : r + 256, :].astype(F32)
        a[r : r + 256, :] = (wide * scale_of(wide)).astype(BF16)


def forward(x, w_gate, w_up, w_down):
    (t, d), ff = x.shape, w_gate.shape[2]
    nt, mt = 512, 512
    n, m = ff // nt, t // mt
    kinds = [w_gate, w_up, w_down] * 2

    def body(x, *refs):
        shards, (mg, mu, hid, h1, a1, a0), full = refs[:6], refs[6:12], refs[12:18]
        a, hidden, tiles, wd, asem, tsem, wsem, *sems = refs[18:]
        here, i = Here(), pl.program_id(0)
        jobs = []
        for k, which in enumerate(((0, 1), (2,), (3, 4), (5,))):
            jobs.append(Gather(here, [(shards[q], full[q]) for q in which], sems[5 * k : 5 * k + 5]))
        first, second, third, fourth = (job.stage for job in jobs)
        keep = pltpu.make_async_copy(a, a0, asem)
        take = pltpu.make_async_copy(full[2], wd, wsem)

        def tile(k, act):
            at = pl.ds(pl.multiple_of(k * nt, nt), nt)
            for q in range(2):
                getattr(pltpu.make_async_copy(full[q].at[:, :, :, at], tiles.at[k % 2, q], tsem.at[k % 2, q]), act)()

        @pl.when(i == 0)
        def _():
            here.meet()
            first(0)
            norm_into(x, a)
            keep.start()
            first(1)
            first(2)
            second(0)
            first(3)
            first(4)
            tile(i, "start")

        @pl.when(i == 1)
        def _():
            second(1)

        @pl.when(i == 2)
        def _():
            second(2)
            third(0)

        @pl.when(i == 3)
        def _():
            second(3)

        @pl.when(i == 4)
        def _():
            second(4)
            take.start()
            third(1)

        @pl.when(i == n + 1)
        def _():
            take.wait()
            third(2)
            fourth(0)

        @pl.when((i >= 1) & (i <= n))
        def _():
            k = i - 1
            tile(k, "wait")

            @pl.when(k < n - 1)
            def _():
                tile(k + 1, "start")

            wg, wu = (tiles[k % 2, q].reshape(d, nt) for q in range(2))
            for r in range(0, t, mt):
                at = slice(r, r + mt)
                act, mg[at, :], mu[at, :] = activation(dot(a[at, :], wg, 1, 0), dot(a[at, :], wu, 1, 0))
                act = act.astype(BF16)
                hid[at, :] = act
                hidden[at, pl.ds(pl.multiple_of(k * nt, nt), nt)] = act

        @pl.when(i > n)
        def _():
            at = pl.ds(pl.multiple_of((i - n - 1) * mt, mt), mt)
            out = dot(hidden[at, :], wd[...].reshape(ff, d), 1, 0).astype(BF16).astype(F32)
            after = (x[at, :].astype(F32) + out).astype(BF16)
            h1[...] = after
            norm_into(after, a1)

        @pl.when(i == n + m)
        def _():
            keep.wait()
            third(3)
            fourth(1)
            third(4)
            for s in (2, 3, 4):
                fourth(s)

    late = lambda i: jnp.maximum(i - n - 1, 0)
    tile = pl.BlockSpec((t, nt), lambda i: (0, jnp.clip(i - 1, 0, n - 1)))
    row = pl.BlockSpec((mt, d), lambda i: (late(i), 0))
    ins = [whole(t, d)]
    for k, w in enumerate(kinds):
        ins.append(pl.BlockSpec((1,) + w.shape[1:], lambda i, k=k: (k // 3, 0, 0), pipeline_mode=pl.Buffered(1)))
    gathered = [S((8, 2) + w.shape[1:], BF16) for w in kinds]
    out = call(
        body, "forward", 1 + n + m, ins, [tile, tile, tile, row, row, ANY] + [ANY] * 6,
        [S((t, ff), F32)] * 2 + [S((t, ff), BF16)] + [S((t, d), BF16)] * 3 + gathered,
        [pltpu.VMEM((t, d), BF16), pltpu.VMEM((t, ff), BF16), pltpu.VMEM((2, 2, 8, 2, d // 16, nt), BF16),
         pltpu.VMEM((8, 2, ff // 16, d), BF16), DMA, DMA((2, 2)), DMA]
        + Gather.scratch(2) + Gather.scratch(1) + Gather.scratch(2) + Gather.scratch(1),
        [x, *kinds], 6 * t * d * ff, 0,
    )
    return *out[:6], *(w.reshape(-1, w.shape[-1]) for w in out[6:])


def activation(g, u):
    s = 0.5 * jnp.tanh(0.5 * g) + 0.5
    silu = g * s
    return silu * u, u * (s + silu * (1 - s)), silu


def last_layer(a, wg, wu, wd, g, name, **job):
    t, d = a.shape
    ff, nt, mt = wd.shape[0], 512, 512

    def compute(a, wg, wu, wd, y, bgu, by_wd, hidden):
        for at in (slice(r0, r0 + mt) for r0 in range(0, t, mt)):
            hid, mg, mu = activation(dot(a[at, :], wg[...], 1, 0), dot(a[at, :], wu[...], 1, 0))
            hidden[at, :] = hid.astype(BF16)
            b = dot(y[at, :], wd[...], 1, 1).astype(BF16).astype(F32)
            bgu[0, at, :] = (b * mg).astype(BF16)
            bgu[1, at, :] = (b * mu).astype(BF16)
        by_wd[...] = dot(hidden[...], y[...], 0, 0).astype(BF16)

    return fused(
        name, ff // nt, compute, [whole(t, d), columns(d, nt), columns(d, nt), rows(nt, d), whole(t, d)],
        [pl.BlockSpec((2, t, nt), lambda i: (0, 0, i)), rows(nt, d)], [S((2, t, ff), BF16), S((ff, d), BF16)],
        [pltpu.VMEM((t, nt), BF16)], [a, wg, wu, wd, g], 8 * t * d * ff, **job,
    )


def by_hidden(g, wd, by_g, by_u, hidden, name, **job):
    t, d = g.shape
    ff, nt, mt = wd.shape[0], 512, 512

    def compute(y, wd, mg, mu, hidden, bgu, by_wd):
        for at in (slice(r0, r0 + mt) for r0 in range(0, t, mt)):
            b = dot(y[at, :], wd[...], 1, 1).astype(BF16).astype(F32)
            bgu[0, at, :] = (b * mg[at, :]).astype(BF16)
            bgu[1, at, :] = (b * mu[at, :]).astype(BF16)
        by_wd[...] = dot(hidden[...], y[...], 0, 0).astype(BF16)

    tile = columns(t, nt)
    return fused(
        name, ff // nt, compute, [whole(t, d), rows(nt, d), tile, tile, tile],
        [pl.BlockSpec((2, t, nt), lambda i: (0, 0, i)), rows(nt, d)], [S((2, t, ff), BF16), S((ff, d), BF16)], [],
        [g, wd, by_g, by_u, hidden], 4 * t * d * ff, **job,
    )


def layer_end(a, bgu, wg, wu, h, g, by_wd, name, cid, plans):
    t, d = h.shape
    ff, nt, mt, r = bgu.shape[2], 512, 256, d // 16
    n = ff // nt
    first, second = 2 * n, t // mt
    last = first + second - 1

    hold = len(plans) == 2

    def body(a, cols, both, wg, wu, h, g, by_wd, out, dwd, dwg, *refs):
        dwu, (kgu, ggu, tmp, keep, ksem, *bufs) = refs[: 1 + hold], refs[1 + hold :]
        i, here, per = pl.program_id(0), Here(), Scatter.PER
        mats = [
            (keep, lambda j: by_wd.at[here.chips[j] * 2 + here.other], dwd),
            (kgu.at[0], lambda j: ggu.at[0, j], dwg),
            (kgu.at[1], lambda j: ggu.at[1, j], dwu[0]),
        ]
        jobs = [Scatter(here, [mats[k]], bufs[k * per : (k + 1) * per]) for k in range(len(plans))]
        own = [pltpu.make_async_copy(by_wd.at[here.chips[j] * 2 + here.core], keep.at[j], ksem.at[j]) for j in range(8)]
        kept = [pltpu.make_async_copy(src.at[1], dst, ksem.at[q]) for q, (src, dst) in enumerate(zip((kgu, ggu), dwu))]

        @pl.when(i == 0)
        def _():
            for copy in own:
                copy.start()
            here.meet()

        @pl.when(i == 1)
        def _():
            for copy in own:
                copy.wait()

        if hold:

            @pl.when(i == first)
            def _():
                for copy in kept:
                    copy.start()

        for job, plan in zip(jobs, plans):
            at_steps(here, job, [s if s <= last else -1 for s in plan], False)

        @pl.when(i < first)
        def _():
            w = dot(a[...], cols[0], 0, 0).astype(BF16)
            for c in range(16):
                tmp[c // 2, c % 2] = w[c * r : (c + 1) * r, :]
            at = pl.ds(pl.multiple_of((i % n) * nt, nt), nt)
            for j in range(8):
                kgu[i // n, j, :, at] = tmp[here.chips[j], here.core]
                ggu[i // n, j, :, at] = tmp[here.chips[j], here.other]

        @pl.when(i >= first)
        def _():
            b = (dot(both[0], wg[...], 1, 1) + dot(both[1], wu[...], 1, 1)).astype(BF16).astype(F32)
            wide = h[...].astype(F32)
            s = scale_of(wide)
            along = jnp.mean(b * wide, -1, keepdims=True)
            back = (s * (b - wide * (s * s * along))).astype(BF16).astype(F32)
            out[...] = (g[...].astype(F32) + back).astype(BF16)

        for s in range(5):
            for job, plan in zip(jobs, plans):
                if plan[s] > last:
                    at_steps(here, job, [last if q == s else -1 for q in range(5)], False)
        if hold:

            @pl.when(i == last)
            def _():
                for copy in kept:
                    copy.wait()

    late = lambda i: jnp.maximum(i - first, 0)
    row = pl.BlockSpec((mt, d), lambda i: (late(i), 0))
    early = lambda i: jnp.minimum(i, first - 1)
    shapes = [(by_wd.shape[0] // 16, d), (r, ff), (r, ff)][: len(plans)]
    blocks = by_wd.reshape(16, -1, d)
    return call(
        body, name, first + second,
        [
            whole(t, d),
            pl.BlockSpec((1, t, nt), lambda i: (early(i) // n, 0, early(i) % n)),
            pl.BlockSpec((2, mt, ff), lambda i: (0, late(i), 0)),
            whole(d, ff), whole(d, ff), row, row, ANY,
        ],
        [row] + [whole(*s) for s in shapes] + [ANY, ANY] * hold,
        [S((t, d), BF16)] + [S(s, BF16) for s in shapes] + [S((8, r, ff), BF16)] * (2 * hold),
        [pltpu.VMEM((2, 8, r, ff), BF16), pltpu.VMEM((2, 8, r, ff), BF16), pltpu.VMEM((8, 2, r, nt), BF16),
         pltpu.VMEM((8,) + shapes[0], BF16), DMA((8,))] + Scatter.scratch(shapes),
        [a, bgu, bgu, wg, wu, h, g, blocks], 8 * t * d * ff, cid,
    )


def solution(mesh):
    def step(x, dy, w_gate, w_up, w_down):
        x, g = x[0], dy[0]
        mg0, mu0, hid0, h1, a1, a0, wg0, wu0, wd0, wg1, wu1, wd1 = forward(x, w_gate, w_up, w_down)
        bgu1, by_wd1 = last_layer(a1, wg1, wu1, wd1, g, "last")
        plan_d, plan_g = [0, 2, 5, 8, 10], [5, 7, 11, 13, 15]
        g, dwd1, dwg1, ku1, gu1 = layer_end(a1, bgu1, wg1, wu1, h1, g, by_wd1, "end1", 3, [plan_d, plan_g])
        bgu0, by_wd0, dwu1 = by_hidden(g, wd0, mg0, mu0, hid0, "dh0", cid=5, scatter=[(ku1, gu1)], steps=[0, 1, 2, 3, 4])
        plan_u = [10, 12, 15, 17, 99]
        g, dwd0, dwg0, dwu0 = layer_end(a0, bgu0, wg0, wu0, x, g, by_wd0, "end0", 4, [plan_d, plan_g, plan_u])
        return g[None], jnp.stack([dwg0, dwg1]), jnp.stack([dwu0, dwu1]), jnp.stack([dwd0, dwd1])

    rows_, cols_, out = P(("rep", "dp")), P(None, "dp"), P("rep", "dp")
    return jax.shard_map(
        step, mesh=mesh, in_specs=(rows_, rows_, cols_, cols_, cols_), out_specs=(rows_, out, out, out), check_vma=False
    )
```

```python
import functools

import jax
import jax.numpy as jnp
from jax import lax
from jax.experimental import pallas as pl
from jax.experimental.pallas import tpu as pltpu
from jax.sharding import PartitionSpec as P

F32, BF16 = jnp.float32, jnp.bfloat16
S = jax.ShapeDtypeStruct
MESH = pl.DeviceIdType.MESH
ANY = pl.BlockSpec(memory_space=pl.ANY)
DMA = pltpu.SemaphoreType.DMA
CUBE = (4, 2, 1)
LIMIT = 67_043_328


def dot(a, b, ca, cb):
    return lax.dot_general(a, b, (((ca,), (cb,)), ((), ())), preferred_element_type=F32)


def whole(*shape):
    return pl.BlockSpec(shape, lambda i: (0,) * len(shape), pipeline_mode=pl.Buffered(1))


def rows(mt, cols):
    return pl.BlockSpec((mt, cols), lambda i: (i, 0))


def columns(n, nt):
    return pl.BlockSpec((n, nt), lambda i: (0, i))


class Here:
    def __init__(self):
        me, rep = lax.axis_index("dp"), lax.axis_index("rep")
        chip, self.core = me // 2, me % 2
        self.at = at = [(chip // d) % 2 for d in CUBE]
        own = [c * d for c, d in zip(at, CUBE)]
        far = [d - o for o, d in zip(own, CUBE)]
        self.other = 1 - self.core
        pick = lambda r: [f if r & d else o for o, f, d in zip(own, far, CUBE)]
        self.chips = [sum(pick(r)[1:], pick(r)[0]) for r in range(8)]
        self.devices = {d: (rep, self.chips[d] * 2 + self.core) for d in CUBE}
        self.devices[0] = (rep, chip * 2 + self.other)

    def meet(self):
        barrier = pltpu.get_barrier_semaphore()
        for d in (*CUBE, 0):
            pl.semaphore_signal(barrier, 1, device_id=self.devices[d], device_id_type=MESH)
        pl.semaphore_wait(barrier, 4)

    def remote(self, src, dst, send, recv, d):
        return pltpu.make_async_remote_copy(
            src_ref=src, dst_ref=dst, send_sem=send, recv_sem=recv, device_id=self.devices[d], device_id_type=MESH
        )


def stripes(cols, first):
    tiles = cols // 128
    cut = [tiles // 3 + (1 if (p + first) % 3 < tiles % 3 else 0) for p in range(3)]
    out, at = [], 0
    for p in range(3):
        out.append((slice(at * 128, (at + cut[p]) * 128), CUBE[p:] + CUBE[:p]))
        at += cut[p]
    return out


class Gather:
    def __init__(self, here, mats, sems):
        self.here = here
        self.mats, (self.send, self.recv, self.dsend, self.drecv, self.local) = mats, sems

    @staticmethod
    def scratch(n):
        return [DMA((n, 3, 7)), DMA((n, 3, 7)), DMA((n, 3, 8)), DMA((n, 3, 8)), DMA((n,))]

    def each(self):
        for m, (src, dst) in enumerate(self.mats):
            for p, (cols, order) in enumerate(stripes(src.shape[-1], m)):
                yield m, p, src, dst, cols, order

    def block(self, item, r, other=False):
        m, p, src, dst, cols, order = item
        here = self.here
        return dst.at[here.chips[r], here.other if other else here.core, :, cols]

    def hop(self, item, j, d):
        m, p, src, dst, cols, order = item
        here = src.at[0, :, cols] if j == 0 else self.block(item, j)
        return self.here.remote(here, self.block(item, j), self.send.at[m, p, (j ^ d) - 1], self.recv.at[m, p, (j ^ d) - 1], d)

    def arrived(self, item, r):
        m, p = item[:2]
        self.here.remote(self.block(item, r), self.block(item, r), self.send.at[m, p, r - 1], self.recv.at[m, p, r - 1], 1).wait_recv()

    def hand(self, item, r):
        m, p, src, dst, cols, order = item
        here = src.at[0, :, cols] if r == 0 else self.block(item, r)
        return self.here.remote(here, self.block(item, r), self.dsend.at[m, p, r], self.drecv.at[m, p, r], 0)

    def stage(self, s):
        items = list(self.each())
        if s == 0:
            for n in range(3):
                for it in items:
                    self.hop(it, 0, it[5][n]).start()
            for it in items:
                self.hand(it, 0).start()
            for m, (src, dst) in enumerate(self.mats):
                pltpu.make_async_copy(src.at[0], dst.at[self.here.chips[0], self.here.core], self.local.at[m]).start()
        if s == 1:
            for it in items:
                d0, d1, d2 = it[5]
                self.arrived(it, d0)
                self.hop(it, d0, d1).start()
                self.hop(it, d0, d2).start()
                self.hand(it, d0).start()
        if s == 2:
            for it in items:
                d0, d1, d2 = it[5]
                for r in (d1, d0 ^ d1):
                    self.arrived(it, r)
                    self.hop(it, r, d2).start()
                    self.hand(it, r).start()
        if s == 3:
            for it in items:
                d0, d1, d2 = it[5]
                for r in (d2, d0 ^ d2, d1 ^ d2, 7):
                    self.arrived(it, r)
                    self.hand(it, r).start()
        if s == 4:
            for it in items:
                m, p = it[:2]
                d0, d1, d2 = it[5]
                for r in range(8):
                    self.here.remote(
                        self.block(it, r, True), self.block(it, r, True), self.dsend.at[m, p, r], self.drecv.at[m, p, r], 0
                    ).wait_recv()
                    self.hand(it, r).wait_send()
                for j, d in ((0, d0), (0, d1), (d0, d1), (0, d2), (d0, d2), (d1, d2), (d0 ^ d1, d2)):
                    self.hop(it, j, d).wait_send()
            for m, (src, dst) in enumerate(self.mats):
                pltpu.make_async_copy(src.at[0], dst.at[self.here.chips[0], self.here.core], self.local.at[m]).wait()


class Scatter:
    def __init__(self, here, mats, bufs):
        self.here, self.mats, self.bufs = here, mats, bufs

    @staticmethod
    def scratch(shapes):
        out = []
        for r, c in shapes:
            out += [pltpu.VMEM((n, r, c), BF16) for n in (8, 4, 2, 1)]
            out += [pltpu.VMEM((n, r, c), BF16) for n in (4, 2, 1)]
            out += [DMA((3, 8)), DMA((3, 8)), DMA((3, 7)), DMA((3, 7))]
        return out

    PER = 11

    def each(self):
        for m, (keep, give, out) in enumerate(self.mats):
            b = self.bufs[m * self.PER : (m + 1) * self.PER]
            for p, (cols, order) in enumerate(stripes(keep.shape[-1], m)):
                yield p, keep, give, out, b[:4], b[4:7], b[7:], cols, order

    @staticmethod
    def groups(order):
        d0, d1, d2 = order
        return [[d1, d1 ^ d2, d2, 0], [d2, 0], [0]]

    def hand(self, it, r):
        p, keep, give, out, inn, leave, sems, cols, order = it
        return self.here.remote(give(r).at[:, cols], inn[0].at[r, :, cols], sems[0].at[p, r], sems[1].at[p, r], 0)

    def hop(self, it, s, n):
        p, keep, give, out, inn, leave, sems, cols, order = it
        k = (0, 4, 6)[s] + n
        return self.here.remote(leave[s].at[n, :, cols], inn[s + 1].at[n, :, cols], sems[2].at[p, k], sems[3].at[p, k], order[s])

    def total(self, it, r, upto):
        p, keep, give, out, inn, leave, sems, cols, order = it
        t = keep[r, :, cols].astype(F32) + inn[0][r, :, cols].astype(F32)
        for s in range(upto):
            t = t + inn[s + 1][self.groups(order)[s].index(r), :, cols].astype(F32)
        return t

    def stage(self, s):
        items = list(self.each())
        if s == 0:
            for first in (True, False):
                for it in items:
                    for r in range(8):
                        if bool(r & it[8][0]) == first:
                            self.hand(it, r).start()
            return
        for it in items:
            out, leave, cols, order = it[3], it[5], it[7], it[8]
            groups, h = self.groups(order), s - 1
            going = [r ^ order[h] for r in groups[h]] if s < 4 else [0]
            for n, r in enumerate(going):
                self.hand(it, r).wait_recv()
                for k in range(h):
                    self.hop(it, k, groups[k].index(r)).wait_recv()
                t = self.total(it, r, h).astype(BF16)
                if s < 4:
                    leave[h][n, :, cols] = t
                    self.hop(it, h, n).start()
                else:
                    out[:, cols] = t
        if s == 4:
            for it in items:
                for r in range(8):
                    self.hand(it, r).wait_send()
                for h, n in ((0, 4), (1, 2), (2, 1)):
                    for k in range(n):
                        self.hop(it, h, k).wait_send()


def at_steps(here, job, steps, meet=True):
    i = pl.program_id(0)
    for step in sorted(set(steps) - {-1}):

        @pl.when(i == step)
        def _(step=step):
            for s, when in enumerate(steps):
                if when == step:
                    if s == 0 and meet:
                        here.meet()
                    job.stage(s)


def call(body, name, grid, ins, outs, shapes, scratch, args, flops, cid=None):
    params = dict(dimension_semantics=("arbitrary",), vmem_limit_bytes=LIMIT)
    if cid is not None:
        params.update(collective_id=cid, has_side_effects=True)
    kw = dict(
        name=name,
        grid=(grid,),
        in_specs=ins,
        out_specs=outs,
        out_shape=shapes,
        scratch_shapes=scratch,
        compiler_params=pltpu.CompilerParams(**params),
        cost_estimate=pl.CostEstimate(flops=flops, bytes_accessed=flops // 500, transcendentals=0),
    )
    return pl.pallas_call(body, **kw)(*args)


def with_job(compute, kind, n_in, n_out, n_scr, mats, steps_of, grid):
    def body(*refs):
        k = mats * (1 if kind is Gather else 2) if kind else 0
        ins, refs = refs[:n_in], refs[n_in:]
        jin, refs = refs[:k], refs[k:]
        outs, refs = refs[:n_out], refs[n_out:]
        jout, refs = refs[:mats], refs[mats:]
        scr, bufs = refs[:n_scr], refs[n_scr:]
        here = Here() if kind else None
        if kind is Gather:
            job = Gather(here, list(zip(jin, jout)), bufs)
        elif kind is Scatter:
            job = Scatter(here, [(k, lambda r, g=g: g.at[r], o) for k, g, o in zip(jin[::2], jin[1::2], jout)], bufs)
        last = grid - 1
        if kind:
            at_steps(here, job, [s if not s % 1 and (s < last or not n) else -1 for n, s in enumerate(steps_of)])
        if compute and any(s % 1 for s in steps_of or ()):
            compute(*ins, *outs, *scr, lambda: at_steps(here, job, [int(s) if s % 1 else -1 for s in steps_of]))
        elif compute:
            compute(*ins, *outs, *scr)
        if kind:
            at_steps(here, job, [s if not s % 1 and s >= last and n else -1 for n, s in enumerate(steps_of)])

    return body


def fused(name, grid, compute, ins, outs, shapes, scratch, args, flops, cid=None, gather=None, scatter=None, steps=None):
    ins, outs, shapes, scratch, args = list(ins), list(outs), list(shapes), list(scratch), list(args)
    n_in, n_out, n_scr, kind, mats = len(ins), len(outs), len(scratch), None, 0
    if gather:
        kind, mats = Gather, len(gather)
        for w, layer in gather:
            r, c = w.shape[1:]
            ins.append(pl.BlockSpec((1, r, c), lambda i, layer=layer: (layer, 0, 0), pipeline_mode=pl.Buffered(1)))
            args.append(w)
            outs.append(ANY)
            shapes.append(S((8, 2, r, c), BF16))
        scratch += Gather.scratch(mats)
    if scatter:
        kind, mats = Scatter, len(scatter)
        for keep, give in scatter:
            ins += [whole(*keep.shape), ANY]
            args += [keep, give]
            outs.append(whole(*keep.shape[1:]))
            shapes.append(S(keep.shape[1:], BF16))
        scratch += Scatter.scratch([k.shape[1:] for k, _ in scatter])
    body = with_job(compute, kind, n_in, n_out, n_scr, mats, steps, grid)
    return call(body, name, grid, ins, outs, shapes, scratch, args, flops, cid)


def scale_of(wide):
    return lax.rsqrt(jnp.mean(wide * wide, -1, keepdims=True) + 1e-6)


def norm_into(h, a):
    for r in range(0, h.shape[0], 256):
        wide = h[r : r + 256, :].astype(F32)
        a[r : r + 256, :] = (wide * scale_of(wide)).astype(BF16)


def forward(x, w_gate, w_up, w_down):
    (t, d), ff = x.shape, w_gate.shape[2]
    nt, mt = 512, 512
    n, m = ff // nt, t // mt
    kinds = [w_gate, w_up, w_down] * 2

    def body(x, *refs):
        shards, (mg, mu, hid, h1, a1, a0), full = refs[:6], refs[6:12], refs[12:18]
        a, hidden, tiles, wd, asem, tsem, wsem, *sems = refs[18:]
        here, i = Here(), pl.program_id(0)
        jobs = []
        for k, which in enumerate(((0, 1), (2,), (3, 4), (5,))):
            jobs.append(Gather(here, [(shards[q], full[q]) for q in which], sems[5 * k : 5 * k + 5]))
        first, second, third, fourth = (job.stage for job in jobs)
        keep = pltpu.make_async_copy(a, a0, asem)
        take = pltpu.make_async_copy(full[2], wd, wsem)

        def tile(k, act):
            at = pl.ds(pl.multiple_of(k * nt, nt), nt)
            for q in range(2):
                getattr(pltpu.make_async_copy(full[q].at[:, :, :, at], tiles.at[k % 2, q], tsem.at[k % 2, q]), act)()

        @pl.when(i == 0)
        def _():
            here.meet()
            first(0)
            norm_into(x, a)
            keep.start()
            first(1)
            first(2)
            second(0)
            first(3)
            first(4)
            tile(i, "start")

        @pl.when(i == 1)
        def _():
            second(1)

        @pl.when(i == 2)
        def _():
            second(2)
            third(0)

        @pl.when(i == 3)
        def _():
            second(3)

        @pl.when(i == 4)
        def _():
            second(4)
            take.start()
            third(1)

        @pl.when(i == n + 1)
        def _():
            take.wait()
            third(2)
            fourth(0)

        @pl.when((i >= 1) & (i <= n))
        def _():
            k = i - 1
            tile(k, "wait")

            @pl.when(k < n - 1)
            def _():
                tile(k + 1, "start")

            wg, wu = (lambda q=q: tiles[k % 2, q].reshape(d, nt) for q in range(2))

            @pl.loop(0, m)
            def _(q):
                at = pl.ds(pl.multiple_of(q * mt, mt), mt)
                act, mg[at, :], mu[at, :] = activation(dot(a[at, :], wg(), 1, 0), dot(a[at, :], wu(), 1, 0))
                act = act.astype(BF16)
                hid[at, :] = act
                hidden[at, pl.ds(pl.multiple_of(k * nt, nt), nt)] = act

        @pl.when(i > n)
        def _():
            at = pl.ds(pl.multiple_of((i - n - 1) * mt, mt), mt)
            out = dot(hidden[at, :], wd[...].reshape(ff, d), 1, 0).astype(BF16).astype(F32)
            after = (x[at, :].astype(F32) + out).astype(BF16)
            h1[...] = after
            norm_into(after, a1)

        @pl.when(i == n + m)
        def _():
            keep.wait()
            third(3)
            fourth(1)
            fourth(2)
            third(4)
            fourth(3)
            fourth(4)

    late = lambda i: jnp.maximum(i - n - 1, 0)
    tile = pl.BlockSpec((t, nt), lambda i: (0, jnp.clip(i - 1, 0, n - 1)))
    row = pl.BlockSpec((mt, d), lambda i: (late(i), 0))
    ins = [whole(t, d)]
    for k, w in enumerate(kinds):
        ins.append(pl.BlockSpec((1,) + w.shape[1:], lambda i, k=k: (k // 3, 0, 0), pipeline_mode=pl.Buffered(1)))
    gathered = [S((8, 2) + w.shape[1:], BF16) for w in kinds]
    out = call(
        body, "forward", 1 + n + m, ins, [tile, tile, tile, row, row, ANY] + [ANY] * 6,
        [S((t, ff), F32)] * 2 + [S((t, ff), BF16)] + [S((t, d), BF16)] * 3 + gathered,
        [pltpu.VMEM((t, d), BF16), pltpu.VMEM((t, ff), BF16), pltpu.VMEM((2, 2, 8, 2, d // 16, nt), BF16),
         pltpu.VMEM((8, 2, ff // 16, d), BF16), DMA, DMA((2, 2)), DMA]
        + Gather.scratch(2) + Gather.scratch(1) + Gather.scratch(2) + Gather.scratch(1),
        [x, *kinds], 6 * t * d * ff, 0,
    )
    return *out[:6], *(w.reshape(-1, w.shape[-1]) for w in out[6:])


def activation(g, u):
    s = 0.5 * jnp.tanh(0.5 * g) + 0.5
    silu = g * s
    return silu * u, u * (s + silu * (1 - s)), silu


def last_layer(a, wg, wu, wd, g, name, **job):
    t, d = a.shape
    ff, nt, mt = wd.shape[0], 512, 512

    def compute(a, wg, wu, wd, y, bgu, by_wd, hidden):
        @pl.loop(0, t // mt)
        def _(q):
            at = pl.ds(pl.multiple_of(q * mt, mt), mt)
            hid, mg, mu = activation(dot(a[at, :], wg[...], 1, 0), dot(a[at, :], wu[...], 1, 0))
            hidden[at, :] = hid.astype(BF16)
            b = dot(y[at, :], wd[...], 1, 1).astype(BF16).astype(F32)
            bgu[0, at, :] = (b * mg).astype(BF16)
            bgu[1, at, :] = (b * mu).astype(BF16)
        by_wd[...] = dot(hidden[...], y[...], 0, 0).astype(BF16)

    return fused(
        name, ff // nt, compute, [whole(t, d), columns(d, nt), columns(d, nt), rows(nt, d), whole(t, d)],
        [pl.BlockSpec((2, t, nt), lambda i: (0, 0, i)), rows(nt, d)], [S((2, t, ff), BF16), S((ff, d), BF16)],
        [pltpu.VMEM((t, nt), BF16)], [a, wg, wu, wd, g], 8 * t * d * ff, **job,
    )


def by_hidden(g, wd, by_g, by_u, hidden, name, **job):
    t, d = g.shape
    ff, nt, mt = wd.shape[0], 512, 512

    def compute(y, wd, mg, mu, hidden, bgu, by_wd, between=None):
        for at in (slice(r0, r0 + mt) for r0 in range(0, t, mt)):
            b = dot(y[at, :], wd[...], 1, 1).astype(BF16).astype(F32)
            bgu[0, at, :] = (b * mg[at, :]).astype(BF16)
            bgu[1, at, :] = (b * mu[at, :]).astype(BF16)
        if between:
            between()
        by_wd[...] = dot(hidden[...], y[...], 0, 0).astype(BF16)

    tile = columns(t, nt)
    return fused(
        name, ff // nt, compute, [whole(t, d), rows(nt, d), tile, tile, tile],
        [pl.BlockSpec((2, t, nt), lambda i: (0, 0, i)), rows(nt, d)], [S((2, t, ff), BF16), S((ff, d), BF16)], [],
        [g, wd, by_g, by_u, hidden], 4 * t * d * ff, **job,
    )


def layer_end(a, bgu, wg, wu, h, g, by_wd, name, cid, plans):
    t, d = h.shape
    ff, nt, mt, r = bgu.shape[2], 512, 256, d // 16
    n = ff // nt
    first, second = 2 * n, t // mt
    last = first + second - 1

    hold = len(plans) == 2

    def body(a, cols, both, wg, wu, h, g, by_wd, out, dwd, dwg, *refs):
        dwu, (kgu, ggu, tmp, keep, ksem, *bufs) = refs[: 1 + hold], refs[1 + hold :]
        i, here, per = pl.program_id(0), Here(), Scatter.PER
        mats = [
            (keep, lambda j: by_wd.at[here.chips[j] * 2 + here.other], dwd),
            (kgu.at[0], lambda j: ggu.at[0, j], dwg),
            (kgu.at[1], lambda j: ggu.at[1, j], dwu[0]),
        ]
        jobs = [Scatter(here, [mats[k]], bufs[k * per : (k + 1) * per]) for k in range(len(plans))]
        own = [pltpu.make_async_copy(by_wd.at[here.chips[j] * 2 + here.core], keep.at[j], ksem.at[j]) for j in range(8)]
        kept = hold and [pltpu.make_async_copy(src.at[1], dst, ksem.at[q]) for q, (src, dst) in enumerate(zip((kgu, ggu), dwu))]

        @pl.when(i == 0)
        def _():
            for copy in own:
                copy.start()
            here.meet()

        @pl.when(i == 1)
        def _():
            for copy in own:
                copy.wait()

        if hold:

            @pl.when(i == first)
            def _():
                for copy in kept:
                    copy.start()

        for job, plan in zip(jobs, plans):
            at_steps(here, job, [s if s <= last else -1 for s in plan], False)

        @pl.when(i < first)
        def _():
            w = dot(a[...], cols[0], 0, 0).astype(BF16)
            for c in range(16):
                tmp[c // 2, c % 2] = w[c * r : (c + 1) * r, :]
            at = pl.ds(pl.multiple_of((i % n) * nt, nt), nt)
            for j in range(8):
                kgu[i // n, j, :, at] = tmp[here.chips[j], here.core]
                ggu[i // n, j, :, at] = tmp[here.chips[j], here.other]

        @pl.when(i >= first)
        def _():
            b = (dot(both[0], wg[...], 1, 1) + dot(both[1], wu[...], 1, 1)).astype(BF16).astype(F32)
            wide = h[...].astype(F32)
            s = scale_of(wide)
            along = jnp.mean(b * wide, -1, keepdims=True)
            back = (s * (b - wide * (s * s * along))).astype(BF16).astype(F32)
            out[...] = (g[...].astype(F32) + back).astype(BF16)

        for s in range(5):
            for job, plan in zip(jobs, plans):
                if plan[s] > last:
                    at_steps(here, job, [last if q == s else -1 for q in range(5)], False)
        if hold:

            @pl.when(i == last)
            def _():
                for copy in kept:
                    copy.wait()

    late = lambda i: jnp.maximum(i - first, 0)
    row = pl.BlockSpec((mt, d), lambda i: (late(i), 0))
    early = lambda i: jnp.minimum(i, first - 1)
    shapes = [(by_wd.shape[0] // 16, d), (r, ff), (r, ff)][: len(plans)]
    blocks = by_wd.reshape(16, -1, d)
    return call(
        body, name, first + second,
        [
            whole(t, d),
            pl.BlockSpec((1, t, nt), lambda i: (early(i) // n, 0, early(i) % n)),
            pl.BlockSpec((2, mt, ff), lambda i: (0, late(i), 0)),
            whole(d, ff), whole(d, ff), row, row, ANY,
        ],
        [row] + [whole(*s) for s in shapes] + [ANY, ANY] * hold,
        [S((t, d), BF16)] + [S(s, BF16) for s in shapes] + [S((8, r, ff), BF16)] * (2 * hold),
        [pltpu.VMEM((2, 8, r, ff), BF16), pltpu.VMEM((2, 8, r, ff), BF16), pltpu.VMEM((8, 2, r, nt), BF16),
         pltpu.VMEM((8,) + shapes[0], BF16), DMA((8,))] + Scatter.scratch(shapes),
        [a, bgu, bgu, wg, wu, h, g, blocks], 8 * t * d * ff, cid,
    )


def results(g, lower, upper):
    (t, d), mt = g.shape, 512
    pairs = list(zip(lower, upper))

    def body(g, *refs):
        out, stacks, ins = refs[6], refs[7:], refs[:6]
        out[0] = g[...]

        @pl.when(pl.program_id(0) == 0)
        def _():
            for k, to in enumerate(stacks):
                to[0], to[1] = ins[2 * k][...], ins[2 * k + 1][...]

    return call(
        body, "results", t // mt, [rows(mt, d)] + [whole(*w.shape) for pair in pairs for w in pair],
        [pl.BlockSpec((1, mt, d), lambda i: (0, i, 0))] + [whole(2, *w.shape) for w in lower],
        [S((1, t, d), BF16)] + [S((2, *w.shape), BF16) for w in lower], [], [g, *(w for pair in pairs for w in pair)], 1000,
    )


def solution(mesh):
    def step(x, dy, w_gate, w_up, w_down):
        x, g = x[0], dy[0]
        mg0, mu0, hid0, h1, a1, a0, wg0, wu0, wd0, wg1, wu1, wd1 = forward(x, w_gate, w_up, w_down)
        bgu1, by_wd1 = last_layer(a1, wg1, wu1, wd1, g, "last")
        plan_d, plan_g = [0, 2, 6, 9, 11], [6, 9, 13, 15, 17]
        g, dwd1, dwg1, ku1, gu1 = layer_end(a1, bgu1, wg1, wu1, h1, g, by_wd1, "end1", 3, [plan_d, plan_g])
        bgu0, by_wd0, dwu1 = by_hidden(g, wd0, mg0, mu0, hid0, "dh0", cid=5, scatter=[(ku1, gu1)], steps=[0, 0.5, 2, 3, 4])
        plan_u = [10, 12, 16, 17, 99]
        g, dwd0, dwg0, dwu0 = layer_end(a0, bgu0, wg0, wu0, x, g, by_wd0, "end0", 4, [plan_d, [5, 7, 11, 13, 15], plan_u])
        return results(g, [dwg0, dwu0, dwd0], [dwg1, dwu1, dwd1])

    rows_, cols_, out = P(("rep", "dp")), P(None, "dp"), P("rep", "dp")
    return jax.shard_map(
        step, mesh=mesh, in_specs=(rows_, rows_, cols_, cols_, cols_), out_specs=(rows_, out, out, out), check_vma=False
    )
```

```python
import functools

import jax
import jax.numpy as jnp
from jax import lax
from jax.experimental import pallas as pl
from jax.experimental.pallas import tpu as pltpu
from jax.sharding import PartitionSpec as P

F32, BF16 = jnp.float32, jnp.bfloat16
S = jax.ShapeDtypeStruct
MESH = pl.DeviceIdType.MESH
ANY = pl.BlockSpec(memory_space=pl.ANY)
DMA = pltpu.SemaphoreType.DMA
CUBE = (4, 2, 1)
LIMIT = 67_043_328


def dot(a, b, ca, cb):
    return lax.dot_general(a, b, (((ca,), (cb,)), ((), ())), preferred_element_type=F32)


def whole(*shape):
    return pl.BlockSpec(shape, lambda i: (0,) * len(shape), pipeline_mode=pl.Buffered(1))


def rows(mt, cols):
    return pl.BlockSpec((mt, cols), lambda i: (i, 0))


def columns(n, nt):
    return pl.BlockSpec((n, nt), lambda i: (0, i))


class Here:
    def __init__(self):
        me, rep = lax.axis_index("dp"), lax.axis_index("rep")
        chip, self.core = me // 2, me % 2
        self.at = at = [(chip // d) % 2 for d in CUBE]
        own = [c * d for c, d in zip(at, CUBE)]
        far = [d - o for o, d in zip(own, CUBE)]
        self.other = 1 - self.core
        pick = lambda r: [f if r & d else o for o, f, d in zip(own, far, CUBE)]
        self.chips = [sum(pick(r)[1:], pick(r)[0]) for r in range(8)]
        self.devices = {d: (rep, self.chips[d] * 2 + self.core) for d in CUBE}
        self.devices[0] = (rep, chip * 2 + self.other)

    def meet(self):
        barrier = pltpu.get_barrier_semaphore()
        for d in (*CUBE, 0):
            pl.semaphore_signal(barrier, 1, device_id=self.devices[d], device_id_type=MESH)
        pl.semaphore_wait(barrier, 4)

    def remote(self, src, dst, send, recv, d):
        return pltpu.make_async_remote_copy(
            src_ref=src, dst_ref=dst, send_sem=send, recv_sem=recv, device_id=self.devices[d], device_id_type=MESH
        )


def stripes(cols, first):
    tiles = cols // 128
    cut = [tiles // 3 + (1 if (p + first) % 3 < tiles % 3 else 0) for p in range(3)]
    out, at = [], 0
    for p in range(3):
        out.append((slice(at * 128, (at + cut[p]) * 128), CUBE[p:] + CUBE[:p]))
        at += cut[p]
    return out


class Gather:
    def __init__(self, here, mats, sems):
        self.here = here
        self.mats, (self.send, self.recv, self.dsend, self.drecv, self.local) = mats, sems

    @staticmethod
    def scratch(n):
        return [DMA((n, 3, 7)), DMA((n, 3, 7)), DMA((n, 3, 8)), DMA((n, 3, 8)), DMA((n,))]

    def each(self):
        for m, (src, dst) in enumerate(self.mats):
            for p, (cols, order) in enumerate(stripes(src.shape[-1], m)):
                yield m, p, src, dst, cols, order

    def block(self, item, r, other=False):
        m, p, src, dst, cols, order = item
        here = self.here
        return dst.at[here.chips[r], here.other if other else here.core, :, cols]

    def hop(self, item, j, d):
        m, p, src, dst, cols, order = item
        here = src.at[0, :, cols] if j == 0 else self.block(item, j)
        return self.here.remote(here, self.block(item, j), self.send.at[m, p, (j ^ d) - 1], self.recv.at[m, p, (j ^ d) - 1], d)

    def arrived(self, item, r):
        m, p = item[:2]
        self.here.remote(self.block(item, r), self.block(item, r), self.send.at[m, p, r - 1], self.recv.at[m, p, r - 1], 1).wait_recv()

    def hand(self, item, r):
        m, p, src, dst, cols, order = item
        here = src.at[0, :, cols] if r == 0 else self.block(item, r)
        return self.here.remote(here, self.block(item, r), self.dsend.at[m, p, r], self.drecv.at[m, p, r], 0)

    def stage(self, s):
        items = list(self.each())
        if s == 0:
            for n in range(3):
                for it in items:
                    self.hop(it, 0, it[5][n]).start()
            for it in items:
                self.hand(it, 0).start()
            for m, (src, dst) in enumerate(self.mats):
                pltpu.make_async_copy(src.at[0], dst.at[self.here.chips[0], self.here.core], self.local.at[m]).start()
        if s == 1:
            for it in items:
                d0, d1, d2 = it[5]
                self.arrived(it, d0)
                self.hop(it, d0, d1).start()
                self.hop(it, d0, d2).start()
                self.hand(it, d0).start()
        if s == 2:
            for it in items:
                d0, d1, d2 = it[5]
                for r in (d1, d0 ^ d1):
                    self.arrived(it, r)
                    self.hop(it, r, d2).start()
                    self.hand(it, r).start()
        if s == 3:
            for it in items:
                d0, d1, d2 = it[5]
                for r in (d2, d0 ^ d2, d1 ^ d2, 7):
                    self.arrived(it, r)
                    self.hand(it, r).start()
        if s == 4:
            for it in items:
                m, p = it[:2]
                d0, d1, d2 = it[5]
                for r in range(8):
                    self.here.remote(
                        self.block(it, r, True), self.block(it, r, True), self.dsend.at[m, p, r], self.drecv.at[m, p, r], 0
                    ).wait_recv()
                    self.hand(it, r).wait_send()
                for j, d in ((0, d0), (0, d1), (d0, d1), (0, d2), (d0, d2), (d1, d2), (d0 ^ d1, d2)):
                    self.hop(it, j, d).wait_send()
            for m, (src, dst) in enumerate(self.mats):
                pltpu.make_async_copy(src.at[0], dst.at[self.here.chips[0], self.here.core], self.local.at[m]).wait()


class Scatter:
    def __init__(self, here, mats, bufs):
        self.here, self.mats, self.bufs = here, mats, bufs

    @staticmethod
    def scratch(shapes):
        out = []
        for r, c in shapes:
            out += [pltpu.VMEM((n, r, c), BF16) for n in (8, 4, 2, 1)]
            out += [pltpu.VMEM((n, r, c), BF16) for n in (4, 2, 1)]
            out += [DMA((3, 8)), DMA((3, 8)), DMA((3, 7)), DMA((3, 7))]
        return out

    PER = 11

    def each(self):
        for m, (keep, give, out) in enumerate(self.mats):
            b = self.bufs[m * self.PER : (m + 1) * self.PER]
            for p, (cols, order) in enumerate(stripes(keep.shape[-1], m)):
                yield p, keep, give, out, b[:4], b[4:7], b[7:], cols, order

    @staticmethod
    def groups(order):
        d0, d1, d2 = order
        return [[d1, d1 ^ d2, d2, 0], [d2, 0], [0]]

    def hand(self, it, r):
        p, keep, give, out, inn, leave, sems, cols, order = it
        return self.here.remote(give(r).at[:, cols], inn[0].at[r, :, cols], sems[0].at[p, r], sems[1].at[p, r], 0)

    def hop(self, it, s, n):
        p, keep, give, out, inn, leave, sems, cols, order = it
        k = (0, 4, 6)[s] + n
        return self.here.remote(leave[s].at[n, :, cols], inn[s + 1].at[n, :, cols], sems[2].at[p, k], sems[3].at[p, k], order[s])

    def total(self, it, r, upto):
        p, keep, give, out, inn, leave, sems, cols, order = it
        t = keep[r, :, cols].astype(F32) + inn[0][r, :, cols].astype(F32)
        for s in range(upto):
            t = t + inn[s + 1][self.groups(order)[s].index(r), :, cols].astype(F32)
        return t

    def stage(self, s):
        items = list(self.each())
        if s == 0:
            for first in (True, False):
                for it in items:
                    for r in range(8):
                        if bool(r & it[8][0]) == first:
                            self.hand(it, r).start()
            return
        for it in items:
            out, leave, cols, order = it[3], it[5], it[7], it[8]
            groups, h = self.groups(order), s - 1
            going = [r ^ order[h] for r in groups[h]] if s < 4 else [0]
            for n, r in enumerate(going):
                self.hand(it, r).wait_recv()
                for k in range(h):
                    self.hop(it, k, groups[k].index(r)).wait_recv()
                t = self.total(it, r, h).astype(BF16)
                if s < 4:
                    leave[h][n, :, cols] = t
                    self.hop(it, h, n).start()
                else:
                    out[:, cols] = t
        if s == 4:
            for it in items:
                for r in range(8):
                    self.hand(it, r).wait_send()
                for h, n in ((0, 4), (1, 2), (2, 1)):
                    for k in range(n):
                        self.hop(it, h, k).wait_send()


def at_steps(here, job, steps, meet=True):
    i = pl.program_id(0)
    for step in sorted(set(steps) - {-1}):

        @pl.when(i == step)
        def _(step=step):
            for s, when in enumerate(steps):
                if when == step:
                    if s == 0 and meet:
                        here.meet()
                    job.stage(s)


def call(body, name, grid, ins, outs, shapes, scratch, args, flops, cid=None):
    params = dict(dimension_semantics=("arbitrary",), vmem_limit_bytes=LIMIT)
    if cid is not None:
        params.update(collective_id=cid, has_side_effects=True)
    kw = dict(
        name=name,
        grid=(grid,),
        in_specs=ins,
        out_specs=outs,
        out_shape=shapes,
        scratch_shapes=scratch,
        compiler_params=pltpu.CompilerParams(**params),
        cost_estimate=pl.CostEstimate(flops=flops, bytes_accessed=flops // 500, transcendentals=0),
    )
    return pl.pallas_call(body, **kw)(*args)


def with_job(compute, kind, n_in, n_out, n_scr, mats, steps_of, grid):
    def body(*refs):
        k = mats * (1 if kind is Gather else 2) if kind else 0
        ins, refs = refs[:n_in], refs[n_in:]
        jin, refs = refs[:k], refs[k:]
        outs, refs = refs[:n_out], refs[n_out:]
        jout, refs = refs[:mats], refs[mats:]
        scr, bufs = refs[:n_scr], refs[n_scr:]
        here = Here() if kind else None
        if kind is Gather:
            job = Gather(here, list(zip(jin, jout)), bufs)
        elif kind is Scatter:
            job = Scatter(here, [(k, lambda r, g=g: g.at[r], o) for k, g, o in zip(jin[::2], jin[1::2], jout)], bufs)
        last = grid - 1
        if kind:
            at_steps(here, job, [s if not s % 1 and (s < last or not n) else -1 for n, s in enumerate(steps_of)])
        if compute and any(s % 1 for s in steps_of or ()):
            compute(*ins, *outs, *scr, lambda: at_steps(here, job, [int(s) if s % 1 else -1 for s in steps_of]))
        elif compute:
            compute(*ins, *outs, *scr)
        if kind:
            at_steps(here, job, [s if not s % 1 and s >= last and n else -1 for n, s in enumerate(steps_of)])

    return body


def fused(name, grid, compute, ins, outs, shapes, scratch, args, flops, cid=None, gather=None, scatter=None, steps=None):
    ins, outs, shapes, scratch, args = list(ins), list(outs), list(shapes), list(scratch), list(args)
    n_in, n_out, n_scr, kind, mats = len(ins), len(outs), len(scratch), None, 0
    if gather:
        kind, mats = Gather, len(gather)
        for w, layer in gather:
            r, c = w.shape[1:]
            ins.append(pl.BlockSpec((1, r, c), lambda i, layer=layer: (layer, 0, 0), pipeline_mode=pl.Buffered(1)))
            args.append(w)
            outs.append(ANY)
            shapes.append(S((8, 2, r, c), BF16))
        scratch += Gather.scratch(mats)
    if scatter:
        kind, mats = Scatter, len(scatter)
        for keep, give in scatter:
            ins += [whole(*keep.shape), ANY]
            args += [keep, give]
            outs.append(whole(*keep.shape[1:]))
            shapes.append(S(keep.shape[1:], BF16))
        scratch += Scatter.scratch([k.shape[1:] for k, _ in scatter])
    body = with_job(compute, kind, n_in, n_out, n_scr, mats, steps, grid)
    return call(body, name, grid, ins, outs, shapes, scratch, args, flops, cid)


def scale_of(wide):
    return lax.rsqrt(jnp.mean(wide * wide, -1, keepdims=True) + 1e-6)


def norm_into(h, a):
    for r in range(0, h.shape[0], 256):
        wide = h[r : r + 256, :].astype(F32)
        a[r : r + 256, :] = (wide * scale_of(wide)).astype(BF16)


EVENTS = {
    0: ((0, 1), (0, 2), (1, 0), (0, 3), (0, 4)),
    1: ((1, 1), (2, 0)),
    2: ((1, 2), (3, 0)),
    4: ((1, 3), (2, 1)),
    5: ((1, 4),),
    6: ((2, 2),),
    7: ((3, 1),),
    9: ((2, 3), (3, 2), (2, 4), (3, 3), (3, 4)),
}


def forward(x, w_gate, w_up, w_down):
    (t, d), ff = x.shape, w_gate.shape[2]
    nt, mt = 512, 512
    n, m = ff // nt, t // mt
    kinds = [w_gate, w_up, w_down] * 2

    def body(x, *refs):
        shards, (mg, mu, hid, h1, a1, a0), full = refs[:6], refs[6:12], refs[12:18]
        a, hidden, tiles, wd, asem, tsem, wsem, *sems = refs[18:]
        here, i = Here(), pl.program_id(0)
        jobs = []
        for k, which in enumerate(((0, 1), (2,), (3, 4), (5,))):
            jobs.append(Gather(here, [(shards[q], full[q]) for q in which], sems[5 * k : 5 * k + 5]))
        first = jobs[0].stage
        keep = pltpu.make_async_copy(a, a0, asem)
        take = pltpu.make_async_copy(full[2], wd, wsem)

        def tile(k, act):
            at = pl.ds(pl.multiple_of(k * nt, nt), nt)
            for q in range(2):
                getattr(pltpu.make_async_copy(full[q].at[:, :, :, at], tiles.at[k % 2, q], tsem.at[k % 2, q]), act)()

        def run(events):
            for job, stage in events:
                jobs[job].stage(stage)

        @pl.when(i == 0)
        def _():
            here.meet()
            first(0)
            norm_into(x, a)
            keep.start()
            run(EVENTS[0])
            tile(i, "start")

        for k in range(1, n + m):
            if k in EVENTS or k in (n, n + 1):

                @pl.when(i == k)
                def _(k=k):
                    run(EVENTS.get(k, ()))
                    if k == n:
                        take.start()
                    if k == n + 1:
                        take.wait()

        @pl.when((i >= 1) & (i <= n))
        def _():
            k = i - 1
            tile(k, "wait")

            @pl.when(k < n - 1)
            def _():
                tile(k + 1, "start")

            wg, wu = (lambda q=q: tiles[k % 2, q].reshape(d, nt) for q in range(2))

            @pl.loop(0, m)
            def _(q):
                at = pl.ds(pl.multiple_of(q * mt, mt), mt)
                act, mg[at, :], mu[at, :] = activation(dot(a[at, :], wg(), 1, 0), dot(a[at, :], wu(), 1, 0))
                act = act.astype(BF16)
                hid[at, :] = act
                hidden[at, pl.ds(pl.multiple_of(k * nt, nt), nt)] = act

        @pl.when(i > n)
        def _():
            at = pl.ds(pl.multiple_of((i - n - 1) * mt, mt), mt)
            out = dot(hidden[at, :], wd[...].reshape(ff, d), 1, 0).astype(BF16).astype(F32)
            after = (x[at, :].astype(F32) + out).astype(BF16)
            h1[...] = after
            norm_into(after, a1)

        @pl.when(i == n + m)
        def _():
            keep.wait()
            run(EVENTS[n + m])

    late = lambda i: jnp.maximum(i - n - 1, 0)
    tile = pl.BlockSpec((t, nt), lambda i: (0, jnp.clip(i - 1, 0, n - 1)))
    row = pl.BlockSpec((mt, d), lambda i: (late(i), 0))
    ins = [whole(t, d)]
    for k, w in enumerate(kinds):
        ins.append(pl.BlockSpec((1,) + w.shape[1:], lambda i, k=k: (k // 3, 0, 0), pipeline_mode=pl.Buffered(1)))
    gathered = [S((8, 2) + w.shape[1:], BF16) for w in kinds]
    out = call(
        body, "forward", 1 + n + m, ins, [tile, tile, tile, row, row, ANY] + [ANY] * 6,
        [S((t, ff), F32)] * 2 + [S((t, ff), BF16)] + [S((t, d), BF16)] * 3 + gathered,
        [pltpu.VMEM((t, d), BF16), pltpu.VMEM((t, ff), BF16), pltpu.VMEM((2, 2, 8, 2, d // 16, nt), BF16),
         pltpu.VMEM((8, 2, ff // 16, d), BF16), DMA, DMA((2, 2)), DMA]
        + Gather.scratch(2) + Gather.scratch(1) + Gather.scratch(2) + Gather.scratch(1),
        [x, *kinds], 6 * t * d * ff, 0,
    )
    return *out[:6], *(w.reshape(-1, w.shape[-1]) for w in out[6:])


def activation(g, u):
    s = 0.5 * jnp.tanh(0.5 * g) + 0.5
    silu = g * s
    return silu * u, u * (s + silu * (1 - s)), silu


def last_layer(a, wg, wu, wd, g, name, **job):
    t, d = a.shape
    ff, nt, mt = wd.shape[0], 512, 1024

    def compute(a, wg, wu, wd, y, bgu, by_wd, hidden):
        @pl.loop(0, t // mt)
        def _(q):
            at = pl.ds(pl.multiple_of(q * mt, mt), mt)
            hid, mg, mu = activation(dot(a[at, :], wg[...], 1, 0), dot(a[at, :], wu[...], 1, 0))
            hidden[at, :] = hid.astype(BF16)
            b = dot(y[at, :], wd[...], 1, 1).astype(BF16).astype(F32)
            bgu[0, at, :] = (b * mg).astype(BF16)
            bgu[1, at, :] = (b * mu).astype(BF16)
        by_wd[...] = dot(hidden[...], y[...], 0, 0).astype(BF16)

    return fused(
        name, ff // nt, compute, [whole(t, d), columns(d, nt), columns(d, nt), rows(nt, d), whole(t, d)],
        [pl.BlockSpec((2, t, nt), lambda i: (0, 0, i)), rows(nt, d)], [S((2, t, ff), BF16), S((ff, d), BF16)],
        [pltpu.VMEM((t, nt), BF16)], [a, wg, wu, wd, g], 8 * t * d * ff, **job,
    )


def by_hidden(g, wd, by_g, by_u, hidden, name, **job):
    t, d = g.shape
    ff, nt, mt = wd.shape[0], 512, 512

    def compute(y, wd, mg, mu, hidden, bgu, by_wd, between=None):
        for at in (slice(r0, r0 + mt) for r0 in range(0, t, mt)):
            b = dot(y[at, :], wd[...], 1, 1).astype(BF16).astype(F32)
            bgu[0, at, :] = (b * mg[at, :]).astype(BF16)
            bgu[1, at, :] = (b * mu[at, :]).astype(BF16)
        if between:
            between()
        by_wd[...] = dot(hidden[...], y[...], 0, 0).astype(BF16)

    tile = columns(t, nt)
    return fused(
        name, ff // nt, compute, [whole(t, d), rows(nt, d), tile, tile, tile],
        [pl.BlockSpec((2, t, nt), lambda i: (0, 0, i)), rows(nt, d)], [S((2, t, ff), BF16), S((ff, d), BF16)], [],
        [g, wd, by_g, by_u, hidden], 4 * t * d * ff, **job,
    )


def layer_end(a, bgu, wg, wu, h, g, by_wd, name, cid, plans):
    t, d = h.shape
    ff, nt, mt, r = bgu.shape[2], 512, 256, d // 16
    n = ff // nt
    first, second = 2 * n, t // mt
    last = first + second

    hold = len(plans) == 2

    def body(a, cols, both, gate_hbm, up_hbm, h, g, by_wd, out, dwd, dwg, *refs):
        dwu, (both_cores, before, wg, wu, wsem, keep, ksem, *bufs) = refs[: 1 + hold], refs[1 + hold :]
        kgu, ggu = both_cores.at[0], both_cores.at[1]
        i, here, per = pl.program_id(0), Here(), Scatter.PER
        mats = [
            (keep, lambda j: by_wd.at[here.chips[j] * 2 + here.other], dwd),
            (kgu.at[0], lambda j: ggu.at[0, j], dwg),
            (kgu.at[1], lambda j: ggu.at[1, j], dwu[0]),
        ]
        jobs = [Scatter(here, [mats[k]], bufs[k * per : (k + 1) * per]) for k in range(len(plans))]
        own = [pltpu.make_async_copy(by_wd.at[here.chips[j] * 2 + here.core], keep.at[j], ksem.at[j]) for j in range(8)]
        weights = [pltpu.make_async_copy(src, dst, wsem.at[q]) for q, (src, dst) in enumerate(((gate_hbm, wg), (up_hbm, wu)))]
        kept = hold and [pltpu.make_async_copy(src.at[1], dst, ksem.at[q]) for q, (src, dst) in enumerate(zip((kgu, ggu), dwu))]

        @pl.when(i == 0)
        def _():
            before[...] = jnp.zeros_like(before)
            for copy in own:
                copy.start()
            for copy in weights:
                copy.start()
            here.meet()

        @pl.when(i == 1)
        def _():
            for copy in own:
                copy.wait()

        if hold:

            @pl.when(i == first)
            def _():
                for copy in kept:
                    copy.start()

        for job, plan in zip(jobs, plans):
            at_steps(here, job, [s if s <= last else -1 for s in plan], False)

        @pl.when(i < first)
        def _():
            w = dot(a[...], cols[0], 0, 0).astype(BF16)
            at = pl.ds(pl.multiple_of((i % n) * nt, nt), nt)
            for c in range(16):
                both_cores[here.other if c % 2 else here.core, i // n, here.chips[c // 2], :, at] = w[c * r : (c + 1) * r, :]

        @pl.when(i == first)
        def _():
            for copy in weights:
                copy.wait()

        def back():
            b, wide = before[...].astype(F32), h[...].astype(F32)
            s = scale_of(wide)
            along = jnp.mean(b * wide, -1, keepdims=True)
            way = (s * (b - wide * (s * s * along))).astype(BF16).astype(F32)
            out[...] = (g[...].astype(F32) + way).astype(BF16)

        @pl.when((i >= first) & (i < last))
        def _():
            back()
            before[...] = (dot(both[0], wg[...], 1, 1) + dot(both[1], wu[...], 1, 1)).astype(BF16)

        @pl.when(i == last)
        def _():
            back()

        for s in range(5):
            for job, plan in zip(jobs, plans):
                if plan[s] > last:
                    at_steps(here, job, [last if q == s else -1 for q in range(5)], False)
        if hold:

            @pl.when(i == last)
            def _():
                for copy in kept:
                    copy.wait()

    late = lambda i: jnp.clip(i - first, 0, second - 1)
    row = pl.BlockSpec((mt, d), lambda i: (jnp.maximum(i - first - 1, 0), 0))
    early = lambda i: jnp.minimum(i, first - 1)
    shapes = [(by_wd.shape[0] // 16, d), (r, ff), (r, ff)][: len(plans)]
    blocks = by_wd.reshape(16, -1, d)
    return call(
        body, name, last + 1,
        [
            whole(t, d),
            pl.BlockSpec((1, t, nt), lambda i: (early(i) // n, 0, early(i) % n)),
            pl.BlockSpec((2, mt, ff), lambda i: (0, late(i), 0)),
            ANY, ANY, row, row, ANY,
        ],
        [row] + [whole(*s) for s in shapes] + [ANY, ANY] * hold,
        [S((t, d), BF16)] + [S(s, BF16) for s in shapes] + [S((8, r, ff), BF16)] * (2 * hold),
        [pltpu.VMEM((2, 2, 8, r, ff), BF16), pltpu.VMEM((mt, d), BF16), pltpu.VMEM((d, ff), BF16), pltpu.VMEM((d, ff), BF16), DMA((2,)),
         pltpu.VMEM((8,) + shapes[0], BF16), DMA((8,))] + Scatter.scratch(shapes),
        [a, bgu, bgu, wg, wu, h, g, blocks], 8 * t * d * ff, cid,
    )


def results(g, lower, upper):
    (t, d), mt = g.shape, 512
    pairs = list(zip(lower, upper))

    def body(g, *refs):
        out, stacks, ins = refs[6], refs[7:], refs[:6]
        out[0] = g[...]

        @pl.when(pl.program_id(0) == 0)
        def _():
            for k, to in enumerate(stacks):
                to[0], to[1] = ins[2 * k][...], ins[2 * k + 1][...]

    return call(
        body, "results", t // mt, [rows(mt, d)] + [whole(*w.shape) for pair in pairs for w in pair],
        [pl.BlockSpec((1, mt, d), lambda i: (0, i, 0))] + [whole(2, *w.shape) for w in lower],
        [S((1, t, d), BF16)] + [S((2, *w.shape), BF16) for w in lower], [], [g, *(w for pair in pairs for w in pair)], 1000,
    )


def solution(mesh):
    def step(x, dy, w_gate, w_up, w_down):
        x, g = x[0], dy[0]
        mg0, mu0, hid0, h1, a1, a0, wg0, wu0, wd0, wg1, wu1, wd1 = forward(x, w_gate, w_up, w_down)
        bgu1, by_wd1 = last_layer(a1, wg1, wu1, wd1, g, "last")
        plan_d, plan_g = [0, 2, 6, 9, 11], [6, 9, 13, 15, 17]
        g, dwd1, dwg1, ku1, gu1 = layer_end(a1, bgu1, wg1, wu1, h1, g, by_wd1, "end1", 3, [plan_d, plan_g])
        bgu0, by_wd0, dwu1 = by_hidden(g, wd0, mg0, mu0, hid0, "dh0", cid=5, scatter=[(ku1, gu1)], steps=[0, 0.5, 2, 3, 4])
        plan_u = [10, 12, 16, 18, 99]
        g, dwd0, dwg0, dwu0 = layer_end(a0, bgu0, wg0, wu0, x, g, by_wd0, "end0", 4, [plan_d, [5, 7, 11, 14, 16], plan_u])
        return results(g, [dwg0, dwu0, dwd0], [dwg1, dwu1, dwd1])

    rows_, cols_, out = P(("rep", "dp")), P(None, "dp"), P("rep", "dp")
    return jax.shard_map(
        step, mesh=mesh, in_specs=(rows_, rows_, cols_, cols_, cols_), out_specs=(rows_, out, out, out), check_vma=False
    )
```

```python
import functools

import jax
import jax.numpy as jnp
from jax import lax
from jax.experimental import pallas as pl
from jax.experimental.pallas import tpu as pltpu
from jax.sharding import PartitionSpec as P

F32, BF16 = jnp.float32, jnp.bfloat16
S = jax.ShapeDtypeStruct
MESH = pl.DeviceIdType.MESH
ANY = pl.BlockSpec(memory_space=pl.ANY)
DMA = pltpu.SemaphoreType.DMA
CUBE = (4, 2, 1)
LIMIT = 67_043_328


def dot(a, b, ca, cb):
    return lax.dot_general(a, b, (((ca,), (cb,)), ((), ())), preferred_element_type=F32)


def whole(*shape):
    return pl.BlockSpec(shape, lambda i: (0,) * len(shape), pipeline_mode=pl.Buffered(1))


def rows(mt, cols):
    return pl.BlockSpec((mt, cols), lambda i: (i, 0))


def columns(n, nt):
    return pl.BlockSpec((n, nt), lambda i: (0, i))


class Here:
    def __init__(self):
        me, rep = lax.axis_index("dp"), lax.axis_index("rep")
        chip, self.core = me // 2, me % 2
        self.at = at = [(chip // d) % 2 for d in CUBE]
        own = [c * d for c, d in zip(at, CUBE)]
        far = [d - o for o, d in zip(own, CUBE)]
        self.other = 1 - self.core
        pick = lambda r: [f if r & d else o for o, f, d in zip(own, far, CUBE)]
        self.chips = [sum(pick(r)[1:], pick(r)[0]) for r in range(8)]
        self.devices = {d: (rep, self.chips[d] * 2 + self.core) for d in CUBE}
        self.devices[0] = (rep, chip * 2 + self.other)

    def meet(self):
        barrier = pltpu.get_barrier_semaphore()
        for d in (*CUBE, 0):
            pl.semaphore_signal(barrier, 1, device_id=self.devices[d], device_id_type=MESH)
        pl.semaphore_wait(barrier, 4)

    def remote(self, src, dst, send, recv, d):
        return pltpu.make_async_remote_copy(
            src_ref=src, dst_ref=dst, send_sem=send, recv_sem=recv, device_id=self.devices[d], device_id_type=MESH
        )


def stripes(cols, first):
    tiles = cols // 128
    cut = [tiles // 3 + (1 if (p + first) % 3 < tiles % 3 else 0) for p in range(3)]
    out, at = [], 0
    for p in range(3):
        out.append((slice(at * 128, (at + cut[p]) * 128), CUBE[p:] + CUBE[:p]))
        at += cut[p]
    return out


class Gather:
    def __init__(self, here, mats, sems):
        self.here = here
        self.mats, (self.send, self.recv, self.dsend, self.drecv, self.local) = mats, sems

    @staticmethod
    def scratch(n):
        return [DMA((n, 3, 7)), DMA((n, 3, 7)), DMA((n, 3, 8)), DMA((n, 3, 8)), DMA((n,))]

    def each(self):
        for m, (src, dst) in enumerate(self.mats):
            for p, (cols, order) in enumerate(stripes(src.shape[-1], m)):
                yield m, p, src, dst, cols, order

    def block(self, item, r, other=False):
        m, p, src, dst, cols, order = item
        here = self.here
        return dst.at[here.chips[r], here.other if other else here.core, :, cols]

    def hop(self, item, j, d):
        m, p, src, dst, cols, order = item
        here = src.at[0, :, cols] if j == 0 else self.block(item, j)
        return self.here.remote(here, self.block(item, j), self.send.at[m, p, (j ^ d) - 1], self.recv.at[m, p, (j ^ d) - 1], d)

    def arrived(self, item, r):
        m, p = item[:2]
        self.here.remote(self.block(item, r), self.block(item, r), self.send.at[m, p, r - 1], self.recv.at[m, p, r - 1], 1).wait_recv()

    def hand(self, item, r):
        m, p, src, dst, cols, order = item
        here = src.at[0, :, cols] if r == 0 else self.block(item, r)
        return self.here.remote(here, self.block(item, r), self.dsend.at[m, p, r], self.drecv.at[m, p, r], 0)

    def stage(self, s):
        items = list(self.each())
        if s == 0:
            for n in range(3):
                for it in items:
                    self.hop(it, 0, it[5][n]).start()
            for it in items:
                self.hand(it, 0).start()
            for m, (src, dst) in enumerate(self.mats):
                pltpu.make_async_copy(src.at[0], dst.at[self.here.chips[0], self.here.core], self.local.at[m]).start()
        if s == 1:
            for it in items:
                d0, d1, d2 = it[5]
                self.arrived(it, d0)
                self.hop(it, d0, d1).start()
                self.hop(it, d0, d2).start()
                self.hand(it, d0).start()
        if s == 2:
            for it in items:
                d0, d1, d2 = it[5]
                for r in (d1, d0 ^ d1):
                    self.arrived(it, r)
                    self.hop(it, r, d2).start()
                    self.hand(it, r).start()
        if s == 3:
            for it in items:
                d0, d1, d2 = it[5]
                for r in (d2, d0 ^ d2, d1 ^ d2, 7):
                    self.arrived(it, r)
                    self.hand(it, r).start()
        if s == 4:
            for it in items:
                m, p = it[:2]
                d0, d1, d2 = it[5]
                for r in range(8):
                    self.here.remote(
                        self.block(it, r, True), self.block(it, r, True), self.dsend.at[m, p, r], self.drecv.at[m, p, r], 0
                    ).wait_recv()
                    self.hand(it, r).wait_send()
                for j, d in ((0, d0), (0, d1), (d0, d1), (0, d2), (d0, d2), (d1, d2), (d0 ^ d1, d2)):
                    self.hop(it, j, d).wait_send()
            for m, (src, dst) in enumerate(self.mats):
                pltpu.make_async_copy(src.at[0], dst.at[self.here.chips[0], self.here.core], self.local.at[m]).wait()


class Scatter:
    def __init__(self, here, mats, bufs):
        self.here, self.mats, self.bufs = here, mats, bufs

    @staticmethod
    def scratch(shapes):
        out = []
        for r, c in shapes:
            out += [pltpu.VMEM((n, r, c), BF16) for n in (8, 4, 2, 1)]
            out += [pltpu.VMEM((n, r, c), BF16) for n in (4, 2, 1)]
            out += [DMA((3, 8)), DMA((3, 8)), DMA((3, 7)), DMA((3, 7))]
        return out

    PER = 11

    def each(self):
        for m, (keep, give, out) in enumerate(self.mats):
            b = self.bufs[m * self.PER : (m + 1) * self.PER]
            for p, (cols, order) in enumerate(stripes(keep.shape[-1], m)):
                yield p, keep, give, out, b[:4], b[4:7], b[7:], cols, order

    @staticmethod
    def groups(order):
        d0, d1, d2 = order
        return [[d1, d1 ^ d2, d2, 0], [d2, 0], [0]]

    def hand(self, it, r):
        p, keep, give, out, inn, leave, sems, cols, order = it
        return self.here.remote(give(r).at[:, cols], inn[0].at[r, :, cols], sems[0].at[p, r], sems[1].at[p, r], 0)

    def hop(self, it, s, n):
        p, keep, give, out, inn, leave, sems, cols, order = it
        k = (0, 4, 6)[s] + n
        return self.here.remote(leave[s].at[n, :, cols], inn[s + 1].at[n, :, cols], sems[2].at[p, k], sems[3].at[p, k], order[s])

    def total(self, it, r, upto):
        p, keep, give, out, inn, leave, sems, cols, order = it
        t = keep[r, :, cols].astype(F32) + inn[0][r, :, cols].astype(F32)
        for s in range(upto):
            t = t + inn[s + 1][self.groups(order)[s].index(r), :, cols].astype(F32)
        return t

    def stage(self, s):
        items = list(self.each())
        if s == 0:
            for first in (True, False):
                for it in items:
                    for r in range(8):
                        if bool(r & it[8][0]) == first:
                            self.hand(it, r).start()
            return
        for it in items:
            out, leave, cols, order = it[3], it[5], it[7], it[8]
            groups, h = self.groups(order), s - 1
            going = [r ^ order[h] for r in groups[h]] if s < 4 else [0]
            for n, r in enumerate(going):
                self.hand(it, r).wait_recv()
                for k in range(h):
                    self.hop(it, k, groups[k].index(r)).wait_recv()
                t = self.total(it, r, h).astype(BF16)
                if s < 4:
                    leave[h][n, :, cols] = t
                    self.hop(it, h, n).start()
                else:
                    out[:, cols] = t
        if s == 4:
            for it in items:
                for r in range(8):
                    self.hand(it, r).wait_send()
                for h, n in ((0, 4), (1, 2), (2, 1)):
                    for k in range(n):
                        self.hop(it, h, k).wait_send()


def at_steps(here, job, steps, meet=True):
    i = pl.program_id(0)
    for step in sorted(set(steps) - {-1}):

        @pl.when(i == step)
        def _(step=step):
            for s, when in enumerate(steps):
                if when == step:
                    if s == 0 and meet:
                        here.meet()
                    job.stage(s)


def call(body, name, grid, ins, outs, shapes, scratch, args, flops, cid=None):
    params = dict(dimension_semantics=("arbitrary",), vmem_limit_bytes=LIMIT)
    if cid is not None:
        params.update(collective_id=cid, has_side_effects=True)
    kw = dict(
        name=name,
        grid=(grid,),
        in_specs=ins,
        out_specs=outs,
        out_shape=shapes,
        scratch_shapes=scratch,
        compiler_params=pltpu.CompilerParams(**params),
        cost_estimate=pl.CostEstimate(flops=flops, bytes_accessed=flops // 500, transcendentals=0),
    )
    return pl.pallas_call(body, **kw)(*args)


def with_job(compute, kind, n_in, n_out, n_scr, mats, steps_of, grid):
    def body(*refs):
        k = mats * (1 if kind is Gather else 2) if kind else 0
        ins, refs = refs[:n_in], refs[n_in:]
        jin, refs = refs[:k], refs[k:]
        outs, refs = refs[:n_out], refs[n_out:]
        jout, refs = refs[:mats], refs[mats:]
        scr, bufs = refs[:n_scr], refs[n_scr:]
        here = Here() if kind else None
        if kind is Gather:
            job = Gather(here, list(zip(jin, jout)), bufs)
        elif kind is Scatter:
            job = Scatter(here, [(k, lambda r, g=g: g.at[r], o) for k, g, o in zip(jin[::2], jin[1::2], jout)], bufs)
        last = grid - 1
        if kind:
            at_steps(here, job, [s if not s % 1 and (s < last or not n) else -1 for n, s in enumerate(steps_of)])
        if compute and any(s % 1 for s in steps_of or ()):
            compute(*ins, *outs, *scr, lambda: at_steps(here, job, [int(s) if s % 1 else -1 for s in steps_of]))
        elif compute:
            compute(*ins, *outs, *scr)
        if kind:
            at_steps(here, job, [s if not s % 1 and s >= last and n else -1 for n, s in enumerate(steps_of)])

    return body


def fused(name, grid, compute, ins, outs, shapes, scratch, args, flops, cid=None, gather=None, scatter=None, steps=None):
    ins, outs, shapes, scratch, args = list(ins), list(outs), list(shapes), list(scratch), list(args)
    n_in, n_out, n_scr, kind, mats = len(ins), len(outs), len(scratch), None, 0
    if gather:
        kind, mats = Gather, len(gather)
        for w, layer in gather:
            r, c = w.shape[1:]
            ins.append(pl.BlockSpec((1, r, c), lambda i, layer=layer: (layer, 0, 0), pipeline_mode=pl.Buffered(1)))
            args.append(w)
            outs.append(ANY)
            shapes.append(S((8, 2, r, c), BF16))
        scratch += Gather.scratch(mats)
    if scatter:
        kind, mats = Scatter, len(scatter)
        for keep, give in scatter:
            ins += [whole(*keep.shape), ANY]
            args += [keep, give]
            outs.append(whole(*keep.shape[1:]))
            shapes.append(S(keep.shape[1:], BF16))
        scratch += Scatter.scratch([k.shape[1:] for k, _ in scatter])
    body = with_job(compute, kind, n_in, n_out, n_scr, mats, steps, grid)
    return call(body, name, grid, ins, outs, shapes, scratch, args, flops, cid)


def scale_of(wide):
    return lax.rsqrt(jnp.mean(wide * wide, -1, keepdims=True) + 1e-6)


def norm_into(h, a):
    for r in range(0, h.shape[0], 256):
        wide = h[r : r + 256, :].astype(F32)
        a[r : r + 256, :] = (wide * scale_of(wide)).astype(BF16)


EVENTS = {
    0: ((0, 1), (0, 2), (1, 0), (0, 3), (0, 4)),
    1: ((1, 1), (2, 0)),
    2: ((1, 2), (3, 0)),
    4: ((1, 3), (2, 1)),
    5: ((1, 4),),
    6: ((2, 2),),
    7: ((3, 1),),
    9: ((2, 3), (3, 2), (2, 4), (3, 3), (3, 4)),
}


def forward(x, w_gate, w_up, w_down):
    (t, d), ff = x.shape, w_gate.shape[2]
    nt, mt = 512, 512
    n, m = ff // nt, t // mt
    kinds = [w_gate, w_up, w_down] * 2

    def body(x_hbm, *refs):
        shards, (mg, mu, hid, h1, a1, a0), full = refs[:6], refs[6:12], refs[12:18]
        x, a, hidden, tiles, wd, xsem, asem, tsem, wsem, *sems = refs[18:]
        here, i = Here(), pl.program_id(0)
        jobs = []
        for k, which in enumerate(((0, 1), (2,), (3, 4), (5,))):
            jobs.append(Gather(here, [(shards[q], full[q]) for q in which], sems[5 * k : 5 * k + 5]))
        first = jobs[0].stage
        bring = pltpu.make_async_copy(x_hbm, x, xsem)
        keep = pltpu.make_async_copy(a, a0, asem)
        take = pltpu.make_async_copy(full[2], wd, wsem)

        def tile(k, act):
            at = pl.ds(pl.multiple_of(k * nt, nt), nt)
            for q in range(2):
                getattr(pltpu.make_async_copy(full[q].at[:, :, :, at], tiles.at[k % 2, q], tsem.at[k % 2, q]), act)()

        def run(events):
            for job, stage in events:
                jobs[job].stage(stage)

        @pl.when(i == 0)
        def _():
            bring.start()
            here.meet()
            first(0)
            bring.wait()
            norm_into(x, a)
            keep.start()
            run(EVENTS[0])
            tile(i, "start")

        for k in range(1, n + m):
            if k in EVENTS or k in (n, n + 1):

                @pl.when(i == k)
                def _(k=k):
                    run(EVENTS.get(k, ()))
                    if k == n:
                        take.start()
                    if k == n + 1:
                        take.wait()

        @pl.when((i >= 1) & (i <= n))
        def _():
            k = i - 1
            tile(k, "wait")

            @pl.when(k < n - 1)
            def _():
                tile(k + 1, "start")

            wg, wu = (lambda q=q: tiles[k % 2, q].reshape(d, nt) for q in range(2))

            @pl.loop(0, m)
            def _(q):
                at = pl.ds(pl.multiple_of(q * mt, mt), mt)
                act, mg[at, :], mu[at, :] = activation(dot(a[at, :], wg(), 1, 0), dot(a[at, :], wu(), 1, 0))
                act = act.astype(BF16)
                hid[at, :] = act
                hidden[at, pl.ds(pl.multiple_of(k * nt, nt), nt)] = act

        @pl.when(i > n)
        def _():
            at = pl.ds(pl.multiple_of((i - n - 1) * mt, mt), mt)
            out = dot(hidden[at, :], wd[...].reshape(ff, d), 1, 0).astype(BF16).astype(F32)
            after = (x[at, :].astype(F32) + out).astype(BF16)
            h1[...] = after
            norm_into(after, a1)

        @pl.when(i == n + m)
        def _():
            keep.wait()
            run(EVENTS[n + m])

    late = lambda i: jnp.maximum(i - n - 1, 0)
    tile = pl.BlockSpec((t, nt), lambda i: (0, jnp.clip(i - 1, 0, n - 1)))
    row = pl.BlockSpec((mt, d), lambda i: (late(i), 0))
    ins = [ANY]
    for k, w in enumerate(kinds):
        ins.append(pl.BlockSpec((1,) + w.shape[1:], lambda i, k=k: (k // 3, 0, 0), pipeline_mode=pl.Buffered(1)))
    gathered = [S((8, 2) + w.shape[1:], BF16) for w in kinds]
    out = call(
        body, "forward", 1 + n + m, ins, [tile, tile, tile, row, row, ANY] + [ANY] * 6,
        [S((t, ff), F32)] * 2 + [S((t, ff), BF16)] + [S((t, d), BF16)] * 3 + gathered,
        [pltpu.VMEM((t, d), BF16), pltpu.VMEM((t, d), BF16), pltpu.VMEM((t, ff), BF16),
         pltpu.VMEM((2, 2, 8, 2, d // 16, nt), BF16), pltpu.VMEM((8, 2, ff // 16, d), BF16), DMA, DMA, DMA((2, 2)), DMA]
        + Gather.scratch(2) + Gather.scratch(1) + Gather.scratch(2) + Gather.scratch(1),
        [x, *kinds], 6 * t * d * ff, 0,
    )
    return *out[:6], *(w.reshape(-1, w.shape[-1]) for w in out[6:])


def activation(g, u):
    s = 0.5 * jnp.tanh(0.5 * g) + 0.5
    silu = g * s
    return silu * u, u * (s + silu * (1 - s)), silu


def last_layer(a, wg, wu, wd, g, name, **job):
    t, d = a.shape
    ff, nt, mt = wd.shape[0], 512, 1024

    def compute(a, wg, wu, wd, y, bgu, by_wd, hidden):
        @pl.loop(0, t // mt)
        def _(q):
            at = pl.ds(pl.multiple_of(q * mt, mt), mt)
            hid, mg, mu = activation(dot(a[at, :], wg[...], 1, 0), dot(a[at, :], wu[...], 1, 0))
            hidden[at, :] = hid.astype(BF16)
            b = dot(y[at, :], wd[...], 1, 1).astype(BF16).astype(F32)
            bgu[0, at, :] = (b * mg).astype(BF16)
            bgu[1, at, :] = (b * mu).astype(BF16)
        by_wd[...] = dot(hidden[...], y[...], 0, 0).astype(BF16)

    return fused(
        name, ff // nt, compute, [whole(t, d), columns(d, nt), columns(d, nt), rows(nt, d), whole(t, d)],
        [pl.BlockSpec((2, t, nt), lambda i: (0, 0, i)), rows(nt, d)], [S((2, t, ff), BF16), S((ff, d), BF16)],
        [pltpu.VMEM((t, nt), BF16)], [a, wg, wu, wd, g], 8 * t * d * ff, **job,
    )


def by_hidden(g, wd, by_g, by_u, hidden, name, **job):
    t, d = g.shape
    ff, nt, mt = wd.shape[0], 512, 512

    def compute(y, wd, mg, mu, hidden, bgu, by_wd, between=None):
        for at in (slice(r0, r0 + mt) for r0 in range(0, t, mt)):
            b = dot(y[at, :], wd[...], 1, 1).astype(BF16).astype(F32)
            bgu[0, at, :] = (b * mg[at, :]).astype(BF16)
            bgu[1, at, :] = (b * mu[at, :]).astype(BF16)
        if between:
            between()
        by_wd[...] = dot(hidden[...], y[...], 0, 0).astype(BF16)

    tile = columns(t, nt)
    return fused(
        name, ff // nt, compute, [whole(t, d), rows(nt, d), tile, tile, tile],
        [pl.BlockSpec((2, t, nt), lambda i: (0, 0, i)), rows(nt, d)], [S((2, t, ff), BF16), S((ff, d), BF16)], [],
        [g, wd, by_g, by_u, hidden], 4 * t * d * ff, **job,
    )


def layer_end(a, bgu, wg, wu, h, g, by_wd, name, cid, plans):
    t, d = h.shape
    ff, nt, mt, r = bgu.shape[2], 512, 256, d // 16
    n = ff // nt
    first, second = 2 * n, t // mt
    last = first + second

    hold = len(plans) == 2

    def body(a, cols, both, gate_hbm, up_hbm, h, g, by_wd, out, dwd, dwg, *refs):
        dwu, (both_cores, before, wg, wu, wsem, keep, ksem, *bufs) = refs[: 1 + hold], refs[1 + hold :]
        kgu, ggu = both_cores.at[0], both_cores.at[1]
        i, here, per = pl.program_id(0), Here(), Scatter.PER
        mats = [
            (keep, lambda j: by_wd.at[here.chips[j] * 2 + here.other], dwd),
            (kgu.at[0], lambda j: ggu.at[0, j], dwg),
            (kgu.at[1], lambda j: ggu.at[1, j], dwu[0]),
        ]
        jobs = [Scatter(here, [mats[k]], bufs[k * per : (k + 1) * per]) for k in range(len(plans))]
        own = [pltpu.make_async_copy(by_wd.at[here.chips[j] * 2 + here.core], keep.at[j], ksem.at[j]) for j in range(8)]
        weights = [pltpu.make_async_copy(src, dst, wsem.at[q]) for q, (src, dst) in enumerate(((gate_hbm, wg), (up_hbm, wu)))]
        kept = hold and [pltpu.make_async_copy(src.at[1], dst, ksem.at[q]) for q, (src, dst) in enumerate(zip((kgu, ggu), dwu))]

        @pl.when(i == 0)
        def _():
            before[...] = jnp.zeros_like(before)
            for copy in own:
                copy.start()
            for copy in weights:
                copy.start()
            here.meet()

        @pl.when(i == 1)
        def _():
            for copy in own:
                copy.wait()

        if hold:

            @pl.when(i == first)
            def _():
                for copy in kept:
                    copy.start()

        for job, plan in zip(jobs, plans):
            at_steps(here, job, [s if s <= last else -1 for s in plan], False)

        @pl.when(i < first)
        def _():
            w = dot(a[...], cols[0], 0, 0).astype(BF16)
            at = pl.ds(pl.multiple_of((i % n) * nt, nt), nt)
            for c in range(16):
                both_cores[here.other if c % 2 else here.core, i // n, here.chips[c // 2], :, at] = w[c * r : (c + 1) * r, :]

        @pl.when(i == first)
        def _():
            for copy in weights:
                copy.wait()

        def back():
            b, wide = before[...].astype(F32), h[...].astype(F32)
            s = scale_of(wide)
            along = jnp.mean(b * wide, -1, keepdims=True)
            way = (s * (b - wide * (s * s * along))).astype(BF16).astype(F32)
            out[...] = (g[...].astype(F32) + way).astype(BF16)

        @pl.when((i >= first) & (i < last))
        def _():
            back()
            before[...] = (dot(both[0], wg[...], 1, 1) + dot(both[1], wu[...], 1, 1)).astype(BF16)

        @pl.when(i == last)
        def _():
            back()

        for s in range(5):
            for job, plan in zip(jobs, plans):
                if plan[s] > last:
                    at_steps(here, job, [last if q == s else -1 for q in range(5)], False)
        if hold:

            @pl.when(i == last)
            def _():
                for copy in kept:
                    copy.wait()

    late = lambda i: jnp.clip(i - first, 0, second - 1)
    row = pl.BlockSpec((mt, d), lambda i: (jnp.maximum(i - first - 1, 0), 0))
    early = lambda i: jnp.minimum(i, first - 1)
    shapes = [(by_wd.shape[0] // 16, d), (r, ff), (r, ff)][: len(plans)]
    blocks = by_wd.reshape(16, -1, d)
    return call(
        body, name, last + 1,
        [
            whole(t, d),
            pl.BlockSpec((1, t, nt), lambda i: (early(i) // n, 0, early(i) % n)),
            pl.BlockSpec((2, mt, ff), lambda i: (0, late(i), 0)),
            ANY, ANY, row, row, ANY,
        ],
        [row] + [whole(*s) for s in shapes] + [ANY, ANY] * hold,
        [S((t, d), BF16)] + [S(s, BF16) for s in shapes] + [S((8, r, ff), BF16)] * (2 * hold),
        [pltpu.VMEM((2, 2, 8, r, ff), BF16), pltpu.VMEM((mt, d), BF16), pltpu.VMEM((d, ff), BF16), pltpu.VMEM((d, ff), BF16), DMA((2,)),
         pltpu.VMEM((8,) + shapes[0], BF16), DMA((8,))] + Scatter.scratch(shapes),
        [a, bgu, bgu, wg, wu, h, g, blocks], 8 * t * d * ff, cid,
    )


def results(g, lower, upper):
    (t, d), mt = g.shape, 512
    pairs = list(zip(lower, upper))

    def body(g, *refs):
        out, stacks, ins = refs[6], refs[7:], refs[:6]
        out[0] = g[...]

        @pl.when(pl.program_id(0) == 0)
        def _():
            for k, to in enumerate(stacks):
                to[0], to[1] = ins[2 * k][...], ins[2 * k + 1][...]

    return call(
        body, "results", t // mt, [rows(mt, d)] + [whole(*w.shape) for pair in pairs for w in pair],
        [pl.BlockSpec((1, mt, d), lambda i: (0, i, 0))] + [whole(2, *w.shape) for w in lower],
        [S((1, t, d), BF16)] + [S((2, *w.shape), BF16) for w in lower], [], [g, *(w for pair in pairs for w in pair)], 1000,
    )


def solution(mesh):
    def step(x, dy, w_gate, w_up, w_down):
        x, g = x[0], dy[0]
        mg0, mu0, hid0, h1, a1, a0, wg0, wu0, wd0, wg1, wu1, wd1 = forward(x, w_gate, w_up, w_down)
        bgu1, by_wd1 = last_layer(a1, wg1, wu1, wd1, g, "last")
        plan_d, plan_g = [0, 2, 6, 9, 11], [6, 9, 13, 15, 17]
        g, dwd1, dwg1, ku1, gu1 = layer_end(a1, bgu1, wg1, wu1, h1, g, by_wd1, "end1", 3, [plan_d, plan_g])
        bgu0, by_wd0, dwu1 = by_hidden(g, wd0, mg0, mu0, hid0, "dh0", cid=5, scatter=[(ku1, gu1)], steps=[0, 0.5, 2, 3, 4])
        plan_u = [10, 12, 16, 18, 99]
        g, dwd0, dwg0, dwu0 = layer_end(a0, bgu0, wg0, wu0, x, g, by_wd0, "end0", 4, [plan_d, [5, 7, 11, 14, 16], plan_u])
        return results(g, [dwg0, dwu0, dwd0], [dwg1, dwu1, dwd1])

    rows_, cols_, out = P(("rep", "dp")), P(None, "dp"), P("rep", "dp")
    return jax.shard_map(
        step, mesh=mesh, in_specs=(rows_, rows_, cols_, cols_, cols_), out_specs=(rows_, out, out, out), check_vma=False
    )
```
